256 devices in a mesh: cols: 64 (over y, z, x_lo), walk: 4 (over x_hi, core).
Axes of the slice: x: 4 (x_hi: 2, x_lo: 2; x = x_hi * 2 + x_lo), y: 4, z: 8, core: 2. Of those that a mesh axis runs over, the one named last changes fastest.
Arguments:
- green_by_column: float32 [4, 4096, 4096], P('walk', 'cols'), parts along dimension 0, may hold values from -1.5 to 1.5
- field: int32 [4, 3, 4096], P('walk'), parts along dimension 0, may hold values from 0 to 1
Outputs:
- wrapped: float32 [4, 4096, 4096], P('walk', 'cols'), parts along dimension 0
The draws below stay inside these ranges and needn't reach their ends.
There are 4 independent parts, one for each index of `walk`. The reference program is written for one: setup_inputs(seed, part) draws one part's arguments, and reference() takes and returns one part's arrays. A program takes and returns all parts, laid end to end along the dimension named above; each array names one. Nothing has to cross between parts.
All inputs are finite; a program needn't handle non-finite values.
Results may differ from the reference program's by a relative error of at most 0.00012.
Values sent between devices are 32-bit elements; how exact they have to be, the bound alone decides.
A program may use at most 64 MiB of HBM per device.

```python
import jax
import jax.numpy as jnp
from jax import lax

LX = 64
LY = 64
WALKERS = 1
SLICES = 3
SITES = 4096


def set_ends(entries, key, smallest, largest):
    shape = entries.shape
    index_at = [jax.random.randint(jax.random.fold_in(key, axis), (), 0, shape[axis]) for axis in range(len(shape))]
    entries = entries.at[tuple(index_at)].set(smallest)
    longest = shape.index(max(shape))
    index_at[longest] = (index_at[longest] + 1) % shape[longest]
    return entries.at[tuple(index_at)].set(largest)


def block_levels(stream_key, dims, pieces, least, top_value):
    def one(dim, blocks):
        heights = jax.random.uniform(jax.random.fold_in(jax.random.fold_in(stream_key, 6), dim), (blocks,), jnp.float32, least / len(pieces), top_value / len(pieces))
        return jnp.repeat(jnp.exp(heights), dims[dim] // blocks).reshape((-1,) + (1,) * (len(dims) - dim - 1))

    level = one(*pieces[0])
    for cut in pieces[1:]:
        level = level * one(*cut)
    return level


def gaussian(stream_key, extent, scale, most, split=(), dtype=jnp.bfloat16):
    drawn = scale * jax.random.normal(stream_key, extent, jnp.float32)
    if split:
        drawn = drawn * block_levels(stream_key, extent, split, -0.22, 0.18)
    return jnp.clip(drawn, -most, most).astype(dtype)


def setup_inputs(seed: int = 0, part: int = 0) -> dict:
    key_list = jax.random.split(jax.random.key(seed), 3)
    own_keys = jax.random.split(jax.random.fold_in(key_list[2], part), 3)
    return {
        "green_by_column": gaussian(own_keys[0], (WALKERS, SITES, SITES), 0.25, 1.5, ((1, 64),), jnp.float32),
        "field": set_ends(jax.random.randint(own_keys[1], (WALKERS, SLICES, SITES), 0, 2), jax.random.fold_in(own_keys[1], 1), 0, 1).astype(jnp.int32),
    }


hop_rate = 0.6
coupling = 0.65373


def kernel(length, growth):
    indices = jnp.arange(length)
    spectrum = jnp.exp(growth * jnp.cos(2.0 * jnp.pi * indices.astype(jnp.float32) / length))
    column = jnp.fft.ifft(spectrum).real.astype(jnp.float32)
    differ = (indices[:, None] - indices[None, :]) % length
    return column[differ]


def reference(green_by_column, field):
    fwd_x = kernel(LX, hop_rate)
    fwd_y = kernel(LY, hop_rate)
    inv_x = kernel(LX, -hop_rate)
    inv_y = kernel(LY, -hop_rate)
    spins = 2.0 * field.astype(jnp.float32) - 1.0
    highest = lax.Precision.HIGHEST

    def advance(inputs_pair):
        green, spin_rows = inputs_pair
        for moment in range(SLICES):
            boost = jnp.exp(coupling * spin_rows[moment])
            green = green * boost[None, :] / boost[:, None]
            blocks = green.reshape(SITES, LX, LY)
            blocks = jnp.einsum("xa,jab->jxb", fwd_x, blocks, precision=highest)
            blocks = jnp.einsum("yb,jxb->jxy", fwd_y, blocks, precision=highest)
            blocks = blocks.reshape(LX, LY, SITES)
            blocks = jnp.einsum("ax,abi->xbi", inv_x, blocks, precision=highest)
            blocks = jnp.einsum("by,xbi->xyi", inv_y, blocks, precision=highest)
            green = blocks.reshape(SITES, SITES)
        return green

    return lax.map(advance, (green_by_column, spins))
```

```python
import jax
import jax.numpy as jnp
import numpy as np
from jax import lax
from jax.experimental import pallas as pl
from jax.experimental.pallas import tpu as pltpu
from jax.sharding import PartitionSpec as P

L = 64
SITES = L * L
SLICES = 3
PEERS = 64
HALF = 32
CHUNKS = 4
PER_CHUNK = HALF // CHUNKS
PITCH_IN = 72
PITCH_OUT = 40
PITCH_X = 72

hop_rate = 0.6
coupling = 0.65373
UP = float(np.exp(coupling))
DOWN = float(np.exp(-coupling))

MESH = pl.DeviceIdType.MESH


def circulant(rate):
    k = np.arange(L)
    spectrum = np.exp(rate * np.cos(2.0 * np.pi * k / L))
    differ = k[:, None] - k[None, :]
    waves = np.cos(2.0 * np.pi * (differ[:, :, None] * k) / L)
    return (waves * spectrum).sum(-1) / L


def high_low(matrix):
    matrix = matrix.astype(np.float32)
    high = matrix.astype(jnp.bfloat16)
    low = (matrix - high.astype(np.float32)).astype(jnp.bfloat16)
    return high, low


def as_left(matrix):
    high, low = high_low(matrix)
    return np.concatenate([high, low, high], axis=1)


def as_right(matrix):
    both = np.kron(np.eye(2), matrix)
    high, low = high_low(both)
    upper = np.concatenate([high, low], axis=1)
    lower = np.concatenate([high, np.zeros_like(low)], axis=1)
    return np.concatenate([upper, lower], axis=0)


def split(values):
    high = values.astype(jnp.bfloat16)
    low = (values - high.astype(jnp.float32)).astype(jnp.bfloat16)
    return high, low


def mix_rows(weights, values):
    high, low = split(values)
    stacked = jnp.concatenate([high, high, low], axis=0)
    return jnp.dot(weights, stacked, preferred_element_type=jnp.float32)


def mix_lanes(values, weights):
    high, low = split(values)
    wide = jnp.concatenate([high, low], axis=1)
    both = jnp.dot(wide, weights, preferred_element_type=jnp.float32)
    return both[:, :128] + both[:, 128:]


def lane(shape):
    return lax.broadcasted_iota(jnp.int32, shape, len(shape) - 1)


def swap_halves(first, second):
    low = lane(first.shape) < 64
    return (
        jnp.where(low, first, pltpu.roll(second, 64, 1)),
        jnp.where(low, pltpu.roll(first, 64, 1), second),
    )


def rows_of_pair(pair):
    first, second = swap_halves(*pair)
    return jnp.concatenate([first, second], axis=0)


def pair_of_rows(rows):
    return swap_halves(rows[:HALF], rows[HALF:])


def beside(tiles):
    return jnp.concatenate(tiles, axis=1)


def kernel(
    green_ref, field_ref, left_ref, last_ref, lanes_ref, right_ref, out_ref,
    held, flags, gain, turn, own_scale, scale_x, scale_y,
    outgoing, arrived, lines, returning, landed,
    load_sems, send_sem, recv_sems, back_send_sem, back_recv_sems,
):
    me = lax.axis_index("cols")
    barrier = pltpu.get_barrier_semaphore()

    loads = [
        pltpu.make_async_copy(
            green_ref.at[:, pl.ds(t * 128, 128)],
            held.at[pl.ds(t * PITCH_IN, L), :],
            load_sems.at[t],
        )
        for t in range(HALF)
    ]
    for load in loads:
        load.start()

    def greet(k, carry):
        pl.semaphore_signal(
            barrier, inc=1, device_id={"cols": lax.rem(me + k, PEERS)}, device_id_type=MESH
        )
        return carry

    lax.fori_loop(1, PEERS, greet, 0)

    for t in range(HALF):
        flags[pl.ds(t, SLICES, stride=HALF), :] = field_ref[:, t * 128 : (t + 1) * 128].astype(jnp.float32)
    low_half = lane((HALF, 128)) < 64
    for moment in range(SLICES):
        bits = flags[moment * HALF : (moment + 1) * HALF, :]
        turned = pltpu.roll(bits, 64, 1)
        even = jnp.where(low_half, bits, turned)
        odd = jnp.where(low_half, turned, bits)
        gain[moment * L : moment * L + HALF, :] = jnp.where(even > 0.5, UP, DOWN)
        gain[moment * L + HALF : (moment + 1) * L, :] = jnp.where(odd > 0.5, UP, DOWN)
        turn[pl.ds(moment * L, HALF, stride=2), :] = bits
        turn[pl.ds(moment * L + 1, HALF, stride=2), :] = turned
    mine = jnp.broadcast_to(turn[pl.ds(me, 1), :], (HALF, 128))
    spot = lax.broadcasted_iota(jnp.int32, (HALF, 128), 0)
    first = jnp.sum(jnp.where(lane((HALF, 128)) == spot, mine, 0.0), axis=1, keepdims=True)
    second = jnp.sum(jnp.where(lane((HALF, 128)) == spot + HALF, mine, 0.0), axis=1, keepdims=True)
    own_bits = jnp.where(low_half, first, second)
    own_scale[...] = jnp.where(own_bits > 0.5, DOWN, UP)

    for load in loads:
        load.wait()

    def send_out(chunk):
        def one(k, carry):
            peer = lax.rem(me + k, PEERS)
            pltpu.make_async_remote_copy(
                src_ref=outgoing.at[pl.ds(pl.multiple_of(peer * PITCH_OUT + chunk * PER_CHUNK, 8), PER_CHUNK), :],
                dst_ref=arrived.at[me, pl.ds(pl.multiple_of(chunk * PER_CHUNK, 8), PER_CHUNK), :],
                send_sem=send_sem,
                recv_sem=recv_sems.at[me],
                device_id={"cols": peer},
                device_id_type=MESH,
            ).start()
            return carry

        lax.fori_loop(1, PEERS, one, 0)

    def left_chunk(chunk):
        base = chunk * PER_CHUNK
        tiles = []
        for k in range(PER_CHUNK):
            pair = (
                held[pl.ds(base + k, HALF, stride=PITCH_IN), :],
                held[pl.ds(base + k + HALF, HALF, stride=PITCH_IN), :],
            )
            tiles.append(rows_of_pair(pair))
        for moment in range(SLICES):
            scale = gain[moment * L : (moment + 1) * L, :]
            pairs = []
            for k in range(0, PER_CHUNK, 2):
                pairs.append(jnp.concatenate([tiles[k] * scale, tiles[k + 1] * scale], axis=0))
            pairs = [mix_lanes(pair, lanes_ref[...]) for pair in pairs]
            weights = last_ref if moment == SLICES - 1 else left_ref
            mixed = [mix_rows(weights[...], beside([pair[:L], pair[L:]])) for pair in pairs]
            tiles = [half for pair in mixed for half in (pair[:, :128], pair[:, 128:])]
        for k in range(PER_CHUNK):
            row = own_scale[pl.ds(base + k, 1), :]
            outgoing[pl.ds(base + k, L, stride=PITCH_OUT), :] = tiles[k] * row

    def left_step(chunk, carry):
        left_chunk(chunk)

        @pl.when(chunk == 0)
        def _():
            pl.semaphore_wait(barrier, PEERS - 1)

        send_out(chunk)
        return carry

    lax.fori_loop(0, CHUNKS, left_step, 0)

    arrived[me] = outgoing[pl.ds(pl.multiple_of(me * PITCH_OUT, 8), HALF), :]

    def spread(k, carry):
        at = lane((128, 128))
        pick_y = jnp.where(at < 64, k, k + HALF)
        pick_x = jnp.where(at < 64, 2 * k, 2 * k + 1)
        from_row = lax.broadcasted_iota(jnp.int32, (128, 128), 0)
        hot_y = (from_row == pick_y).astype(jnp.bfloat16)
        hot_x = (from_row == pick_x).astype(jnp.bfloat16)
        wide_y = jnp.dot(turn[L : 2 * L, :].astype(jnp.bfloat16), hot_y, preferred_element_type=jnp.float32)
        wide_x = jnp.dot(turn[3 * L : 4 * L, :].astype(jnp.bfloat16), hot_x, preferred_element_type=jnp.float32)
        scale_x[k] = jnp.where(wide_y > 0.5, DOWN, UP)
        scale_y[k] = jnp.where(wide_x > 0.5, DOWN, UP)
        return carry

    square = jnp.concatenate([turn[2 * L : 3 * L, :], jnp.zeros((L, 128), jnp.float32)], axis=0)
    turn[3 * L : 4 * L, :] = square.T[:L, :]
    lax.fori_loop(0, HALF, spread, 0)

    weights = right_ref
    group = 4

    def wait_block(sems, buffer, peer):
        @pl.when(peer != me)
        def _():
            pltpu.make_async_remote_copy(
                src_ref=buffer.at[peer],
                dst_ref=buffer.at[peer],
                send_sem=send_sem,
                recv_sem=sems.at[peer],
                device_id={"cols": peer},
                device_id_type=MESH,
            ).wait_recv()

    def by_lines(step, carry):
        spots = [lax.rem(me // 2 + 2 * HALF - step * group - k, HALF) for k in range(group)]
        for spot in spots:
            for q in range(2):
                wait_block(recv_sems, arrived, 2 * spot + q)
        tiles = [rows_of_pair((arrived[2 * spot], arrived[2 * spot + 1])) for spot in spots]
        mixed = [mix_rows(weights[...], beside(tiles[k : k + 2])) for k in range(0, group, 2)]
        tiles = [half for pair in mixed for half in (pair[:, :128], pair[:, 128:])]
        for spot, tile in zip(spots, tiles):
            even, odd = pair_of_rows(tile)
            lines[pl.ds(2 * spot, HALF, stride=PITCH_X), :] = even
            lines[pl.ds(2 * spot + 1, HALF, stride=PITCH_X), :] = odd
        return carry

    lax.fori_loop(0, HALF // group, by_lines, 0)

    def across(step, carry):
        spots = [step * group + k for k in range(group)]
        tiles = [lines[pl.ds(pl.multiple_of(spot * PITCH_X, 8), L), :] for spot in spots]
        mixed = [mix_rows(weights[...], beside(tiles[k : k + 2])) for k in range(0, group, 2)]
        scaled = [
            pair * beside([scale_x[spots[2 * k]], scale_x[spots[2 * k + 1]]]) for k, pair in enumerate(mixed)
        ]
        mixed = [mix_rows(weights[...], pair) for pair in scaled]
        tiles = [half for pair in mixed for half in (pair[:, :128], pair[:, 128:])]
        for spot, tile in zip(spots, tiles):
            lines[pl.ds(pl.multiple_of(spot * PITCH_X, 8), L), :] = tile
        return carry

    lax.fori_loop(0, HALF // group, across, 0)

    def along(step, carry):
        spots = [step * group + k for k in range(group)]
        tiles = [
            rows_of_pair(
                (
                    lines[pl.ds(2 * spot, HALF, stride=PITCH_X), :],
                    lines[pl.ds(2 * spot + 1, HALF, stride=PITCH_X), :],
                )
            )
            for spot in spots
        ]
        mixed = [mix_rows(weights[...], beside(tiles[k : k + 2])) for k in range(0, group, 2)]
        scaled = [
            pair * beside([scale_y[spots[2 * k]], scale_y[spots[2 * k + 1]]]) for k, pair in enumerate(mixed)
        ]
        mixed = [mix_rows(weights[...], pair) for pair in scaled]
        tiles = [half for pair in mixed for half in (pair[:, :128], pair[:, 128:])]
        for spot, tile in zip(spots, tiles):
            even, odd = pair_of_rows(tile)
            lines[pl.ds(2 * spot, HALF, stride=PITCH_X), :] = even
            lines[pl.ds(2 * spot + 1, HALF, stride=PITCH_X), :] = odd
        return carry

    lax.fori_loop(0, HALF // group, along, 0)

    def send_back(chunk):
        def one(k, carry):
            peer = lax.rem(me + k, PEERS)
            pltpu.make_async_remote_copy(
                src_ref=returning.at[pl.ds(pl.multiple_of(peer * PITCH_OUT + chunk * PER_CHUNK, 8), PER_CHUNK), :],
                dst_ref=landed.at[me, pl.ds(pl.multiple_of(chunk * PER_CHUNK, 8), PER_CHUNK), :],
                send_sem=back_send_sem,
                recv_sem=back_recv_sems.at[me],
                device_id={"cols": peer},
                device_id_type=MESH,
            ).start()
            return carry

        lax.fori_loop(1, PEERS, one, 0)

    def finish(chunk, carry):
        base = chunk * PER_CHUNK
        tiles = [lines[pl.ds(pl.multiple_of((base + k) * PITCH_X, 8), L), :] for k in range(PER_CHUNK)]
        mixed = [mix_rows(weights[...], beside(tiles[k : k + 2])) for k in range(0, PER_CHUNK, 2)]
        tiles = [half for pair in mixed for half in (pair[:, :128], pair[:, 128:])]
        for k, tile in enumerate(tiles):
            returning[pl.ds(base + k, L, stride=PITCH_OUT), :] = tile
        send_back(chunk)
        return carry

    lax.fori_loop(0, CHUNKS, finish, 0)

    landed[me] = returning[pl.ds(pl.multiple_of(me * PITCH_OUT, 8), HALF), :]

    def merge(step, carry):
        spot = lax.rem(me // 2 + 2 * HALF - step, HALF)
        for q in range(2):
            wait_block(back_recv_sems, landed, 2 * spot + q)
        upper, lower = swap_halves(landed[2 * spot], landed[2 * spot + 1])
        columns = pl.ds(pl.multiple_of(spot * 128, 128), 128)
        out_ref[0:HALF, columns] = upper
        out_ref[HALF:L, columns] = lower
        return carry

    lax.fori_loop(0, HALF, merge, 0)

    for buffer, sem in ((arrived, send_sem), (landed, back_send_sem)):
        everything = buffer.at[pl.ds(0, PEERS - 1)]
        pltpu.make_async_remote_copy(
            src_ref=everything,
            dst_ref=everything,
            send_sem=sem,
            recv_sem=recv_sems.at[0],
            device_id={"cols": lax.rem(me + 1, PEERS)},
            device_id_type=MESH,
        ).wait_send()


def shards(green_by_column, field):
    green = green_by_column.reshape(L, SITES)
    bits = field.reshape(SLICES, SITES)
    order = np.concatenate([np.arange(0, L, 2), np.arange(1, L, 2)])
    forward = circulant(hop_rate)
    inverse = circulant(-hop_rate)
    left = jnp.asarray(as_left(forward[np.ix_(order, order)]))
    last = jnp.asarray(as_left(forward[:, order]))
    lanes = jnp.asarray(as_right(forward))
    right = jnp.asarray(as_left(inverse))
    vmem = pl.BlockSpec(memory_space=pltpu.VMEM)
    wrapped = pl.pallas_call(
        kernel,
        out_shape=jax.ShapeDtypeStruct((L, SITES), jnp.float32),
        in_specs=[pl.BlockSpec(memory_space=pl.ANY)] + [vmem] * 5,
        out_specs=vmem,
        scratch_shapes=[
            pltpu.VMEM((HALF * PITCH_IN, 128), jnp.float32),
            pltpu.VMEM((SLICES * HALF, 128), jnp.float32),
            pltpu.VMEM((SLICES * L, 128), jnp.float32),
            pltpu.VMEM((4 * L, 128), jnp.float32),
            pltpu.VMEM((HALF, 128), jnp.float32),
            pltpu.VMEM((HALF, L, 128), jnp.float32),
            pltpu.VMEM((HALF, L, 128), jnp.float32),
            pltpu.VMEM((PEERS * PITCH_OUT, 128), jnp.float32),
            pltpu.VMEM((PEERS, HALF, 128), jnp.float32),
            pltpu.VMEM((HALF * PITCH_X, 128), jnp.float32),
            pltpu.VMEM((PEERS * PITCH_OUT, 128), jnp.float32),
            pltpu.VMEM((PEERS, HALF, 128), jnp.float32),
            pltpu.SemaphoreType.DMA((HALF,)),
            pltpu.SemaphoreType.DMA,
            pltpu.SemaphoreType.DMA((PEERS,)),
            pltpu.SemaphoreType.DMA,
            pltpu.SemaphoreType.DMA((PEERS,)),
        ],
        compiler_params=pltpu.CompilerParams(collective_id=0, has_side_effects=True),
    )(green, bits, left, last, lanes, right)
    return wrapped.reshape(1, L, SITES)


def solution(mesh):
    return jax.shard_map(
        shards,
        mesh=mesh,
        in_specs=(P("walk", "cols", None), P("walk", None, None)),
        out_specs=P("walk", "cols", None),
        check_vma=False,
    )
```

```python
import jax
import jax.numpy as jnp
import numpy as np
from jax import lax
from jax.experimental import pallas as pl
from jax.experimental.pallas import tpu as pltpu
from jax.sharding import PartitionSpec as P

L = 64
SITES = L * L
SLICES = 3
PEERS = 64
TILES = SITES // 128
BLOCKS = 4
ROWS = L // BLOCKS
HALVES = 2
STEPS = 4
PER_STEP = ROWS // STEPS
PITCH_IN = 72
PITCH_OUT = 24
PITCH_X = 72

hop_rate = 0.6
coupling = 0.65373
UP = float(np.exp(coupling))
DOWN = float(np.exp(-coupling))

MESH = pl.DeviceIdType.MESH


def circulant(rate):
    k = np.arange(L)
    spectrum = np.exp(rate * np.cos(2.0 * np.pi * k / L))
    differ = k[:, None] - k[None, :]
    waves = np.cos(2.0 * np.pi * (differ[:, :, None] * k) / L)
    return (waves * spectrum).sum(-1) / L


def high_low(matrix):
    matrix = matrix.astype(np.float32)
    high = matrix.astype(jnp.bfloat16)
    low = (matrix - high.astype(np.float32)).astype(jnp.bfloat16)
    return high, low


def as_left(matrix):
    high, low = high_low(matrix)
    return np.concatenate([high, low, high], axis=1)


def as_right(matrix, columns):
    both = np.kron(np.eye(2), matrix)[:, columns]
    high, low = high_low(both)
    upper = np.concatenate([high, low], axis=1)
    lower = np.concatenate([high, np.zeros_like(low)], axis=1)
    return np.concatenate([upper, lower], axis=0)


def split(values):
    high = values.astype(jnp.bfloat16)
    low = (values - high.astype(jnp.float32)).astype(jnp.bfloat16)
    return high, low


def mix_rows(weights, values):
    high, low = split(values)
    stacked = jnp.concatenate([high, high, low], axis=0)
    return jnp.dot(weights, stacked, preferred_element_type=jnp.float32)


def mix_lanes(values, weights):
    high, low = split(values)
    wide = jnp.concatenate([high, low], axis=1)
    both = jnp.dot(wide, weights, preferred_element_type=jnp.float32)
    return both[:, :128] + both[:, 128:]


def lane(shape):
    return lax.broadcasted_iota(jnp.int32, shape, len(shape) - 1)


def swap_lanes(first, second, width):
    keep = (lane(first.shape) // width) % 2 == 0
    return (
        jnp.where(keep, first, pltpu.roll(second, width, 1)),
        jnp.where(keep, pltpu.roll(first, 128 - width, 1), second),
    )


def swap_blocks(tiles):
    t0, t2 = swap_lanes(tiles[0], tiles[2], 64)
    t1, t3 = swap_lanes(tiles[1], tiles[3], 64)
    t0, t1 = swap_lanes(t0, t1, 32)
    t2, t3 = swap_lanes(t2, t3, 32)
    return [t0, t1, t2, t3]


def rows_of_tiles(tiles):
    return jnp.concatenate(swap_blocks(tiles), axis=0)


def tiles_of_rows(rows):
    return swap_blocks([rows[k * ROWS : (k + 1) * ROWS] for k in range(BLOCKS)])


def beside(tiles):
    return jnp.concatenate(tiles, axis=1)


def mix_tiles(weights, tiles):
    mixed = [mix_rows(weights, beside(tiles[k : k + 2])) for k in range(0, len(tiles), 2)]
    return [half for pair in mixed for half in (pair[:, :128], pair[:, 128:])]


def kernel(
    green_ref, field_ref, left_ref, last_ref, lanes_ref, lanes_last_ref, right_ref, out_ref,
    held, gain, turn, own_scale, scale_x, scale_y,
    outgoing, arrived, lines, returning, landed,
    load_sems, send_sem, recv_sems, back_send_sem, back_recv_sems,
):
    me = lax.axis_index("cols")
    barrier = pltpu.get_barrier_semaphore()

    loads = [
        pltpu.make_async_copy(
            green_ref.at[:, pl.ds(t * 128, 128)],
            held.at[pl.ds(t * PITCH_IN, L), :],
            load_sems.at[t],
        )
        for t in range(TILES)
    ]
    for load in loads:
        load.start()

    def greet(k, carry):
        pl.semaphore_signal(
            barrier, inc=1, device_id={"cols": lax.rem(me + k, PEERS)}, device_id_type=MESH
        )
        return carry

    lax.fori_loop(1, PEERS, greet, 0)

    low_half = lane((TILES, 128)) < 64
    for moment in range(SLICES):
        bits = field_ref[moment * TILES : (moment + 1) * TILES, :].astype(jnp.float32)
        turned = pltpu.roll(bits, 64, 1)
        even = jnp.where(low_half, bits, turned)
        odd = jnp.where(low_half, turned, bits)
        gain[moment * L : moment * L + TILES, :] = jnp.where(even > 0.5, UP, DOWN)
        gain[moment * L + TILES : (moment + 1) * L, :] = jnp.where(odd > 0.5, UP, DOWN)
        turn[pl.ds(moment * L, TILES, stride=2), :] = bits
        turn[pl.ds(moment * L + 1, TILES, stride=2), :] = turned
    mine = jnp.broadcast_to(turn[pl.ds(me, 1), :], (ROWS, 128))
    site = lane((ROWS, 128))
    spot_row = lax.broadcasted_iota(jnp.int32, (ROWS, 128), 0)
    own_bits = jnp.zeros((ROWS, 128), jnp.float32)
    for block in range(BLOCKS):
        picked = jnp.where(site == spot_row + block * ROWS, mine, 0.0)
        own_bits = jnp.where(site // 32 == block, jnp.sum(picked, axis=1, keepdims=True), own_bits)
    own_scale[...] = jnp.where(own_bits > 0.5, DOWN, UP)

    for load in loads:
        load.wait()

    def send_out(half, start, count):
        def one(k, carry):
            peer = lax.rem(me + k, PEERS)
            pltpu.make_async_remote_copy(
                src_ref=outgoing.at[pl.ds(pl.multiple_of((half * PEERS + peer) * PITCH_OUT + start, 8), count), :],
                dst_ref=arrived.at[half * PEERS + me, pl.ds(start, count), :],
                send_sem=send_sem,
                recv_sem=recv_sems.at[half * PEERS + me],
                device_id={"cols": peer},
                device_id_type=MESH,
            ).start()
            return carry

        lax.fori_loop(1, PEERS, one, 0)

    def left_step(step, carry):
        base = step * PER_STEP
        tiles = []
        for k in range(PER_STEP):
            for upper in range(2):
                row = base + k + upper * 2 * ROWS
                pair = swap_lanes(
                    held[pl.ds(row, TILES, stride=PITCH_IN), :],
                    held[pl.ds(row + ROWS, TILES, stride=PITCH_IN), :],
                    64,
                )
                tiles.append(jnp.concatenate(pair, axis=0))
        for moment in range(SLICES):
            ends = moment == SLICES - 1
            scale = gain[moment * L : (moment + 1) * L, :]
            tiles = mix_tiles((last_ref if ends else left_ref)[...], [tile * scale for tile in tiles])
            weights = (lanes_last_ref if ends else lanes_ref)[...]
            pairs = [
                mix_lanes(jnp.concatenate(tiles[k : k + 2], axis=0), weights) for k in range(0, len(tiles), 2)
            ]
            tiles = [part for pair in pairs for part in (pair[:L], pair[L:])]
        for k in range(PER_STEP):
            row = own_scale[pl.ds(base + k, 1), :]
            for half, tile in enumerate(swap_lanes(tiles[2 * k], tiles[2 * k + 1], 64)):
                outgoing[pl.ds(half * PEERS * PITCH_OUT + base + k, L, stride=PITCH_OUT), :] = tile * row
        return carry

    lax.fori_loop(0, STEPS // 2, left_step, 0)
    pl.semaphore_wait(barrier, PEERS - 1)
    send_out(0, 0, ROWS // 2)
    lax.fori_loop(STEPS // 2, STEPS, left_step, 0)
    send_out(0, ROWS // 2, ROWS // 2)
    send_out(1, 0, ROWS)

    for half in range(HALVES):
        arrived[half * PEERS + me] = outgoing[pl.ds(pl.multiple_of((half * PEERS + me) * PITCH_OUT, 8), ROWS), :]

    square = jnp.concatenate([turn[2 * L : 3 * L, :], jnp.zeros((L, 128), jnp.float32)], axis=0)
    turn[3 * L : 4 * L, :] = square.T[:L, :]

    def spread(k, carry):
        block = lane((128, 128)) // 32
        from_row = lax.broadcasted_iota(jnp.int32, (128, 128), 0)
        hot_y = (from_row == block * ROWS + k).astype(jnp.bfloat16)
        hot_x = (from_row == block + k * BLOCKS).astype(jnp.bfloat16)
        wide_y = jnp.dot(turn[L : 2 * L, :].astype(jnp.bfloat16), hot_y, preferred_element_type=jnp.float32)
        wide_x = jnp.dot(turn[3 * L : 4 * L, :].astype(jnp.bfloat16), hot_x, preferred_element_type=jnp.float32)
        scale_x[k] = jnp.where(wide_y > 0.5, DOWN, UP)
        scale_y[k] = jnp.where(wide_x > 0.5, DOWN, UP)
        return carry

    lax.fori_loop(0, ROWS, spread, 0)

    def wait_block(sems, buffer, half, peer):
        @pl.when(peer != me)
        def _():
            at = half * PEERS + peer
            pltpu.make_async_remote_copy(
                src_ref=buffer.at[at],
                dst_ref=buffer.at[at],
                send_sem=send_sem,
                recv_sem=sems.at[at],
                device_id={"cols": peer},
                device_id_type=MESH,
            ).wait_recv()

    group = 8

    def right_half(half, carry):
        weights = right_ref[...]

        def store_lines(spots, tiles):
            for spot, rows in zip(spots, tiles):
                for k, tile in enumerate(tiles_of_rows(rows)):
                    lines[pl.ds(spot * BLOCKS + k, ROWS, stride=PITCH_X), :] = tile

        def by_lines(step, carry):
            spots = [lax.rem(me // BLOCKS + 2 * ROWS - step * group - k, ROWS) for k in range(group)]
            for spot in spots:
                for k in range(BLOCKS):
                    wait_block(recv_sems, arrived, half, spot * BLOCKS + k)
            tiles = [
                rows_of_tiles([arrived[half * PEERS + spot * BLOCKS + k] for k in range(BLOCKS)]) for spot in spots
            ]
            store_lines(spots, mix_tiles(weights, tiles))
            return carry

        lax.fori_loop(0, ROWS // group, by_lines, 0)

        def across(step, carry):
            spots = [step * group + k for k in range(group)]
            tiles = [lines[pl.ds(pl.multiple_of(spot * PITCH_X, 8), L), :] for spot in spots]
            tiles = mix_tiles(weights, tiles)
            tiles = mix_tiles(weights, [tile * scale_x[spot] for spot, tile in zip(spots, tiles)])
            for spot, tile in zip(spots, tiles):
                lines[pl.ds(pl.multiple_of(spot * PITCH_X, 8), L), :] = tile
            return carry

        lax.fori_loop(0, ROWS // group, across, 0)

        def along(step, carry):
            spots = [step * group + k for k in range(group)]
            tiles = [
                rows_of_tiles([lines[pl.ds(spot * BLOCKS + k, ROWS, stride=PITCH_X), :] for k in range(BLOCKS)])
                for spot in spots
            ]
            tiles = mix_tiles(weights, tiles)
            tiles = mix_tiles(weights, [tile * scale_y[spot] for spot, tile in zip(spots, tiles)])
            store_lines(spots, tiles)
            return carry

        lax.fori_loop(0, ROWS // group, along, 0)

        def finish(step, carry):
            spots = [step * group + k for k in range(group)]
            tiles = [lines[pl.ds(pl.multiple_of(spot * PITCH_X, 8), L), :] for spot in spots]
            for spot, tile in zip(spots, mix_tiles(weights, tiles)):
                returning[pl.ds(half * PEERS * PITCH_OUT + spot, L, stride=PITCH_OUT), :] = tile
            return carry

        lax.fori_loop(0, ROWS // group, finish, 0)

        def send_back(k, carry):
            peer = lax.rem(me + k, PEERS)
            pltpu.make_async_remote_copy(
                src_ref=returning.at[pl.ds(pl.multiple_of((half * PEERS + peer) * PITCH_OUT, 8), ROWS), :],
                dst_ref=landed.at[half * PEERS + me],
                send_sem=back_send_sem,
                recv_sem=back_recv_sems.at[half * PEERS + me],
                device_id={"cols": peer},
                device_id_type=MESH,
            ).start()
            return carry

        lax.fori_loop(1, PEERS, send_back, 0)
        landed[half * PEERS + me] = returning[pl.ds(pl.multiple_of((half * PEERS + me) * PITCH_OUT, 8), ROWS), :]
        return carry

    lax.fori_loop(0, HALVES, right_half, 0)

    together = 4

    def merge(step, carry):
        spots = [lax.rem(me // 2 + 2 * TILES - step * together - k, TILES) for k in range(together)]
        for spot in spots:
            for q in range(2):
                for half in range(HALVES):
                    wait_block(back_recv_sems, landed, half, 2 * spot + q)
        for spot in spots:
            tiles = [landed[half * PEERS + 2 * spot + q] for q in range(2) for half in range(HALVES)]
            columns = pl.ds(pl.multiple_of(spot * 128, 128), 128)
            for k, tile in enumerate(swap_blocks(tiles)):
                out_ref[k * ROWS : (k + 1) * ROWS, columns] = tile
        return carry

    lax.fori_loop(0, TILES // together, merge, 0)

    for buffer, sem in ((arrived, send_sem), (landed, back_send_sem)):
        everything = buffer.at[pl.ds(0, HALVES * (PEERS - 1))]
        pltpu.make_async_remote_copy(
            src_ref=everything,
            dst_ref=everything,
            send_sem=sem,
            recv_sem=recv_sems.at[0],
            device_id={"cols": lax.rem(me + 1, PEERS)},
            device_id_type=MESH,
        ).wait_send()


def shards(green_by_column, field):
    green = green_by_column.reshape(L, SITES)
    bits = field.reshape(SLICES * TILES, 128)
    order = np.concatenate([np.arange(0, L, 2), np.arange(1, L, 2)])
    columns = np.arange(128).reshape(2, HALVES, 32).transpose(1, 0, 2).reshape(128)
    forward = circulant(hop_rate)
    inverse = circulant(-hop_rate)
    left = jnp.asarray(as_left(forward[np.ix_(order, order)]))
    last = jnp.asarray(as_left(forward[:, order]))
    lanes = jnp.asarray(as_right(forward, np.arange(128)))
    lanes_last = jnp.asarray(as_right(forward, columns))
    right = jnp.asarray(as_left(inverse))
    vmem = pl.BlockSpec(memory_space=pltpu.VMEM)
    wrapped = pl.pallas_call(
        kernel,
        out_shape=jax.ShapeDtypeStruct((L, SITES), jnp.float32),
        in_specs=[pl.BlockSpec(memory_space=pl.ANY)] + [vmem] * 6,
        out_specs=vmem,
        scratch_shapes=[
            pltpu.VMEM((TILES * PITCH_IN, 128), jnp.float32),
            pltpu.VMEM((SLICES * L, 128), jnp.float32),
            pltpu.VMEM((4 * L, 128), jnp.float32),
            pltpu.VMEM((ROWS, 128), jnp.float32),
            pltpu.VMEM((ROWS, L, 128), jnp.float32),
            pltpu.VMEM((ROWS, L, 128), jnp.float32),
            pltpu.VMEM((HALVES * PEERS * PITCH_OUT, 128), jnp.float32),
            pltpu.VMEM((HALVES * PEERS, ROWS, 128), jnp.float32),
            pltpu.VMEM((ROWS * PITCH_X, 128), jnp.float32),
            pltpu.VMEM((HALVES * PEERS * PITCH_OUT, 128), jnp.float32),
            pltpu.VMEM((HALVES * PEERS, ROWS, 128), jnp.float32),
            pltpu.SemaphoreType.DMA((TILES,)),
            pltpu.SemaphoreType.DMA,
            pltpu.SemaphoreType.DMA((HALVES * PEERS,)),
            pltpu.SemaphoreType.DMA,
            pltpu.SemaphoreType.DMA((HALVES * PEERS,)),
        ],
        compiler_params=pltpu.CompilerParams(collective_id=0, has_side_effects=True),
    )(green, bits, left, last, lanes, lanes_last, right)
    return wrapped.reshape(1, L, SITES)


def solution(mesh):
    return jax.shard_map(
        shards,
        mesh=mesh,
        in_specs=(P("walk", "cols", None), P("walk", None, None)),
        out_specs=P("walk", "cols", None),
        check_vma=False,
    )
```

```python
import jax
import jax.numpy as jnp
import numpy as np
from jax import lax
from jax.experimental import pallas as pl
from jax.experimental.pallas import tpu as pltpu
from jax.sharding import PartitionSpec as P

L = 64
SITES = L * L
SLICES = 3
PEERS = 64
TILES = SITES // 128
BLOCKS = 4
ROWS = L // BLOCKS
HALVES = 2
STEPS = 2
PER_STEP = ROWS // STEPS
GROUP = 8
MERGED = 4
PITCH_IN = 72
PITCH_OUT = 24
PITCH_X = 72

hop_rate = 0.6
coupling = 0.65373
UP = float(np.exp(coupling))
DOWN = float(np.exp(-coupling))

MESH = pl.DeviceIdType.MESH


def circulant(rate):
    k = np.arange(L)
    spectrum = np.exp(rate * np.cos(2.0 * np.pi * k / L))
    differ = k[:, None] - k[None, :]
    waves = np.cos(2.0 * np.pi * (differ[:, :, None] * k) / L)
    return (waves * spectrum).sum(-1) / L


def high_low(matrix):
    matrix = matrix.astype(np.float32)
    high = matrix.astype(jnp.bfloat16)
    low = (matrix - high.astype(np.float32)).astype(jnp.bfloat16)
    return high, low


def as_left(matrix):
    high, low = high_low(matrix)
    return np.concatenate([high, low, high], axis=1)


def as_right(matrix, columns):
    both = np.kron(np.eye(2), matrix)[:, columns]
    high, low = high_low(both)
    upper = np.concatenate([high, low], axis=1)
    lower = np.concatenate([high, np.zeros_like(low)], axis=1)
    return np.concatenate([upper, lower], axis=0)


def split(values):
    high = values.astype(jnp.bfloat16)
    low = (values - high.astype(jnp.float32)).astype(jnp.bfloat16)
    return high, low


def mix_rows(weights, values):
    high, low = split(values)
    stacked = jnp.concatenate([high, high, low], axis=0)
    return jnp.dot(weights, stacked, preferred_element_type=jnp.float32)


def mix_lanes(values, weights):
    high, low = split(values)
    wide = jnp.concatenate([high, low], axis=1)
    both = jnp.dot(wide, weights, preferred_element_type=jnp.float32)
    return both[:, :128] + both[:, 128:]


def lane(shape):
    return lax.broadcasted_iota(jnp.int32, shape, len(shape) - 1)


def swap_lanes(first, second, width):
    keep = (lane(first.shape) // width) % 2 == 0
    return (
        jnp.where(keep, first, pltpu.roll(second, width, 1)),
        jnp.where(keep, pltpu.roll(first, 128 - width, 1), second),
    )


def swap_blocks(tiles):
    t0, t2 = swap_lanes(tiles[0], tiles[2], 64)
    t1, t3 = swap_lanes(tiles[1], tiles[3], 64)
    t0, t1 = swap_lanes(t0, t1, 32)
    t2, t3 = swap_lanes(t2, t3, 32)
    return [t0, t1, t2, t3]


def rows_of_tiles(tiles):
    return jnp.concatenate(swap_blocks(tiles), axis=0)


def tiles_of_rows(rows):
    return swap_blocks([rows[k * ROWS : (k + 1) * ROWS] for k in range(BLOCKS)])


def beside(tiles):
    return jnp.concatenate(tiles, axis=1)


def mix_tiles(weights, tiles):
    mixed = [mix_rows(weights, beside(tiles[k : k + 2])) for k in range(0, len(tiles), 2)]
    return [half for pair in mixed for half in (pair[:, :128], pair[:, 128:])]


def kernel(
    green_ref, field_hbm, left_hbm, last_hbm, lanes_hbm, lanes_last_hbm, right_hbm, out_ref,
    field_ref, left_ref, last_ref, lanes_ref, lanes_last_ref, right_ref, held, gain, turn, own_scale, scale_x, scale_y,
    outgoing, arrived, lines, returning, landed,
    small_sems, load_sem, send_sem, recv_sems, back_send_sem, back_recv_sems,
):
    me = lax.axis_index("cols")
    barrier = pltpu.get_barrier_semaphore()

    loads = [
        pltpu.make_async_copy(
            green_ref.at[:, pl.ds(t * 128, 128)],
            held.at[pl.ds(t * PITCH_IN, L), :],
            load_sem,
        )
        for t in range(TILES)
    ]
    smalls = [
        pltpu.make_async_copy(source, target, small_sems.at[k])
        for k, (source, target) in enumerate(
            [
                (field_hbm, field_ref),
                (left_hbm, left_ref),
                (lanes_hbm, lanes_ref),
                (last_hbm, last_ref),
                (lanes_last_hbm, lanes_last_ref),
                (right_hbm, right_ref),
            ]
        )
    ]
    smalls[0].start()
    for load in loads:
        load.start()
    for small in smalls[1:]:
        small.start()

    def greet(k, carry):
        pl.semaphore_signal(
            barrier, inc=1, device_id={"cols": lax.rem(me + k, PEERS)}, device_id_type=MESH
        )
        return carry

    lax.fori_loop(1, PEERS, greet, 0)

    smalls[0].wait()
    low_half = lane((TILES, 128)) < 64
    for moment in range(SLICES):
        bits = field_ref[moment * TILES : (moment + 1) * TILES, :].astype(jnp.float32)
        turned = pltpu.roll(bits, 64, 1)
        even = jnp.where(low_half, bits, turned)
        odd = jnp.where(low_half, turned, bits)
        gain[moment * L : moment * L + TILES, :] = jnp.where(even > 0.5, UP, DOWN)
        gain[moment * L + TILES : (moment + 1) * L, :] = jnp.where(odd > 0.5, UP, DOWN)
        turn[pl.ds(moment * L, TILES, stride=2), :] = bits
        turn[pl.ds(moment * L + 1, TILES, stride=2), :] = turned
    mine = jnp.broadcast_to(turn[pl.ds(me, 1), :], (ROWS, 128))
    site = lane((ROWS, 128))
    spot_row = lax.broadcasted_iota(jnp.int32, (ROWS, 128), 0)
    own_bits = jnp.zeros((ROWS, 128), jnp.float32)
    for block in range(BLOCKS):
        picked = jnp.where(site == spot_row + block * ROWS, mine, 0.0)
        own_bits = jnp.where(site // 32 == block, jnp.sum(picked, axis=1, keepdims=True), own_bits)
    own_scale[...] = jnp.where(own_bits > 0.5, DOWN, UP)

    for small in smalls[1:]:
        small.wait()
    pltpu.make_async_copy(arrived, arrived, load_sem).wait()

    def send_out(half, start, count):
        def one(k, carry):
            peer = lax.rem(me + k, PEERS)
            pltpu.make_async_remote_copy(
                src_ref=outgoing.at[pl.ds(pl.multiple_of((half * PEERS + peer) * PITCH_OUT + start, 8), count), :],
                dst_ref=arrived.at[half * PEERS + me, pl.ds(pl.multiple_of(start, 8), count), :],
                send_sem=send_sem,
                recv_sem=recv_sems.at[half * 2 + lax.rem(peer // BLOCKS + ROWS - me // BLOCKS, ROWS) // GROUP],
                device_id={"cols": peer},
                device_id_type=MESH,
            ).start()
            return carry

        lax.fori_loop(1, PEERS, one, 0)

    def left_step(step, carry):
        base = step * PER_STEP
        tiles = []
        for k in range(PER_STEP):
            for upper in range(2):
                row = base + k + upper * 2 * ROWS
                pair = swap_lanes(
                    held[pl.ds(row, TILES, stride=PITCH_IN), :],
                    held[pl.ds(row + ROWS, TILES, stride=PITCH_IN), :],
                    64,
                )
                tiles.append(jnp.concatenate(pair, axis=0))
        for moment in range(SLICES):
            ends = moment == SLICES - 1
            scale = gain[moment * L : (moment + 1) * L, :]
            tiles = mix_tiles((last_ref if ends else left_ref)[...], [tile * scale for tile in tiles])
            weights = (lanes_last_ref if ends else lanes_ref)[...]
            stack = mix_lanes(jnp.concatenate(tiles, axis=0), weights)
            tiles = [stack[k * L : (k + 1) * L] for k in range(len(tiles))]
        for k in range(PER_STEP):
            row = own_scale[pl.ds(base + k, 1), :]
            for half, tile in enumerate(swap_lanes(tiles[2 * k], tiles[2 * k + 1], 64)):
                outgoing[pl.ds(half * PEERS * PITCH_OUT + base + k, L, stride=PITCH_OUT), :] = tile * row

        @pl.when(step == 0)
        def _():
            pl.semaphore_wait(barrier, PEERS - 1)

        send_out(0, base, PER_STEP)
        return carry

    lax.fori_loop(0, STEPS, left_step, 0)
    send_out(1, 0, ROWS)

    for half in range(HALVES):
        arrived[half * PEERS + me] = outgoing[pl.ds(pl.multiple_of((half * PEERS + me) * PITCH_OUT, 8), ROWS), :]

    square = jnp.concatenate([turn[2 * L : 3 * L, :], jnp.zeros((L, 128), jnp.float32)], axis=0)
    turn[3 * L : 4 * L, :] = square.T[:L, :]

    def spread(k, carry):
        block = lane((128, 128)) // 32
        from_row = lax.broadcasted_iota(jnp.int32, (128, 128), 0)
        hot_y = (from_row == block * ROWS + k).astype(jnp.bfloat16)
        hot_x = (from_row == block + k * BLOCKS).astype(jnp.bfloat16)
        wide_y = jnp.dot(turn[L : 2 * L, :].astype(jnp.bfloat16), hot_y, preferred_element_type=jnp.float32)
        wide_x = jnp.dot(turn[3 * L : 4 * L, :].astype(jnp.bfloat16), hot_x, preferred_element_type=jnp.float32)
        scale_x[k] = jnp.where(wide_y > 0.5, DOWN, UP)
        scale_y[k] = jnp.where(wide_x > 0.5, DOWN, UP)
        return carry

    lax.fori_loop(0, ROWS, spread, 0)

    def wait_blocks(sem, buffer, count):
        blocks = buffer.at[pl.ds(0, count)]
        pltpu.make_async_remote_copy(
            src_ref=blocks,
            dst_ref=blocks,
            send_sem=send_sem,
            recv_sem=sem,
            device_id={"cols": lax.rem(me + 1, PEERS)},
            device_id_type=MESH,
        ).wait_recv()

    def wait_group(sem, buffer, step, count, own):
        @pl.when(step == 0)
        def _():
            wait_blocks(sem, buffer, count - own)

        @pl.when(step != 0)
        def _():
            wait_blocks(sem, buffer, count)

    group = GROUP

    def right_half(half, carry):
        weights = right_ref[...]

        def store_lines(spots, tiles):
            for spot, rows in zip(spots, tiles):
                for k, tile in enumerate(tiles_of_rows(rows)):
                    lines[pl.ds(spot * BLOCKS + k, ROWS, stride=PITCH_X), :] = tile

        def by_lines(step, carry):
            spots = [lax.rem(me // BLOCKS + 2 * ROWS - step * group - k, ROWS) for k in range(group)]
            wait_group(recv_sems.at[half * 2 + step], arrived, step, group * BLOCKS, 1)
            tiles = [
                rows_of_tiles([arrived[half * PEERS + spot * BLOCKS + k] for k in range(BLOCKS)]) for spot in spots
            ]
            store_lines(spots, mix_tiles(weights, tiles))
            return carry

        lax.fori_loop(0, ROWS // group, by_lines, 0)

        def across(step, carry):
            spots = [step * group + k for k in range(group)]
            tiles = [lines[pl.ds(pl.multiple_of(spot * PITCH_X, 8), L), :] for spot in spots]
            tiles = mix_tiles(weights, tiles)
            tiles = mix_tiles(weights, [tile * scale_x[spot] for spot, tile in zip(spots, tiles)])
            for spot, tile in zip(spots, tiles):
                lines[pl.ds(pl.multiple_of(spot * PITCH_X, 8), L), :] = tile
            return carry

        lax.fori_loop(0, ROWS // group, across, 0)

        def along(step, carry):
            spots = [step * group + k for k in range(group)]
            tiles = [
                rows_of_tiles([lines[pl.ds(spot * BLOCKS + k, ROWS, stride=PITCH_X), :] for k in range(BLOCKS)])
                for spot in spots
            ]
            tiles = mix_tiles(weights, tiles)
            tiles = mix_tiles(weights, [tile * scale_y[spot] for spot, tile in zip(spots, tiles)])
            store_lines(spots, tiles)
            return carry

        lax.fori_loop(0, ROWS // group, along, 0)

        def finish(step, carry):
            spots = [step * group + k for k in range(group)]
            tiles = [lines[pl.ds(pl.multiple_of(spot * PITCH_X, 8), L), :] for spot in spots]
            for spot, tile in zip(spots, mix_tiles(weights, tiles)):
                returning[pl.ds(half * PEERS * PITCH_OUT + spot, L, stride=PITCH_OUT), :] = tile
            return carry

        lax.fori_loop(0, ROWS // group, finish, 0)

        def send_back(k, carry):
            peer = lax.rem(me + k, PEERS)
            pltpu.make_async_remote_copy(
                src_ref=returning.at[pl.ds(pl.multiple_of((half * PEERS + peer) * PITCH_OUT, 8), ROWS), :],
                dst_ref=landed.at[half * PEERS + me],
                send_sem=back_send_sem,
                recv_sem=back_recv_sems.at[lax.rem(peer // 2 + TILES - me // 2, TILES) // MERGED],
                device_id={"cols": peer},
                device_id_type=MESH,
            ).start()
            return carry

        lax.fori_loop(1, PEERS, send_back, 0)
        landed[half * PEERS + me] = returning[pl.ds(pl.multiple_of((half * PEERS + me) * PITCH_OUT, 8), ROWS), :]
        return carry

    lax.fori_loop(0, HALVES, right_half, 0)

    def merge(step, carry):
        spots = [lax.rem(me // 2 + 2 * TILES - step * MERGED - k, TILES) for k in range(MERGED)]
        wait_group(back_recv_sems.at[step], landed, step, MERGED * 2 * HALVES, HALVES)
        for spot in spots:
            tiles = [landed[half * PEERS + 2 * spot + q] for q in range(2) for half in range(HALVES)]
            columns = pl.ds(pl.multiple_of(spot * 128, 128), 128)
            for k, tile in enumerate(swap_blocks(tiles)):
                out_ref[k * ROWS : (k + 1) * ROWS, columns] = tile
        return carry

    lax.fori_loop(0, TILES // MERGED, merge, 0)

    for buffer, sem in ((arrived, send_sem), (landed, back_send_sem)):
        everything = buffer.at[pl.ds(0, HALVES * (PEERS - 1))]
        pltpu.make_async_remote_copy(
            src_ref=everything,
            dst_ref=everything,
            send_sem=sem,
            recv_sem=recv_sems.at[0],
            device_id={"cols": lax.rem(me + 1, PEERS)},
            device_id_type=MESH,
        ).wait_send()


def shards(green_by_column, field):
    green = green_by_column.reshape(L, SITES)
    bits = field.reshape(SLICES * TILES, 128)
    order = np.concatenate([np.arange(0, L, 2), np.arange(1, L, 2)])
    columns = np.arange(128).reshape(2, HALVES, 32).transpose(1, 0, 2).reshape(128)
    forward = circulant(hop_rate)
    inverse = circulant(-hop_rate)
    left = jnp.asarray(as_left(forward[np.ix_(order, order)]))
    last = jnp.asarray(as_left(forward[:, order]))
    lanes = jnp.asarray(as_right(forward, np.arange(128)))
    lanes_last = jnp.asarray(as_right(forward, columns))
    right = jnp.asarray(as_left(inverse))
    vmem = pl.BlockSpec(memory_space=pltpu.VMEM)
    wrapped = pl.pallas_call(
        kernel,
        out_shape=pltpu.VMEM((L, SITES), jnp.float32),
        in_specs=[pl.BlockSpec(memory_space=pl.ANY)] * 7,
        out_specs=vmem,
        scratch_shapes=[
            pltpu.VMEM((SLICES * TILES, 128), jnp.int32),
            pltpu.VMEM(left.shape, jnp.bfloat16),
            pltpu.VMEM(last.shape, jnp.bfloat16),
            pltpu.VMEM(lanes.shape, jnp.bfloat16),
            pltpu.VMEM(lanes_last.shape, jnp.bfloat16),
            pltpu.VMEM(right.shape, jnp.bfloat16),
            pltpu.VMEM((TILES * PITCH_IN, 128), jnp.float32),
            pltpu.VMEM((SLICES * L, 128), jnp.float32),
            pltpu.VMEM((4 * L, 128), jnp.float32),
            pltpu.VMEM((ROWS, 128), jnp.float32),
            pltpu.VMEM((ROWS, L, 128), jnp.float32),
            pltpu.VMEM((ROWS, L, 128), jnp.float32),
            pltpu.VMEM((HALVES * PEERS * PITCH_OUT, 128), jnp.float32),
            pltpu.VMEM((HALVES * PEERS, ROWS, 128), jnp.float32),
            pltpu.VMEM((ROWS * PITCH_X, 128), jnp.float32),
            pltpu.VMEM((HALVES * PEERS * PITCH_OUT, 128), jnp.float32),
            pltpu.VMEM((HALVES * PEERS, ROWS, 128), jnp.float32),
            pltpu.SemaphoreType.DMA((6,)),
            pltpu.SemaphoreType.DMA,
            pltpu.SemaphoreType.DMA,
            pltpu.SemaphoreType.DMA((HALVES * ROWS // GROUP,)),
            pltpu.SemaphoreType.DMA,
            pltpu.SemaphoreType.DMA((TILES // MERGED,)),
        ],
        compiler_params=pltpu.CompilerParams(collective_id=0, has_side_effects=True),
    )(green, bits, left, last, lanes, lanes_last, right)
    return wrapped.reshape(1, L, SITES)


def solution(mesh):
    return jax.shard_map(
        shards,
        mesh=mesh,
        in_specs=(P("walk", "cols", None), P("walk", None, None)),
        out_specs=P("walk", "cols", None),
        check_vma=False,
    )
```

```python
import jax
import jax.numpy as jnp
import numpy as np
from jax import lax
from jax.experimental import pallas as pl
from jax.experimental.pallas import tpu as pltpu
from jax.sharding import PartitionSpec as P

L = 64
SITES = L * L
SLICES = 3
PEERS = 64
TILES = SITES // 128
BLOCKS = 4
ROWS = L // BLOCKS
HALVES = 2
STEPS = 2
PER_STEP = ROWS // STEPS
GROUP = 8
MERGED = 4
PITCH_IN = 72
PITCH_OUT = 24
PITCH_X = 72

hop_rate = 0.6
coupling = 0.65373
UP = float(np.exp(coupling))
DOWN = float(np.exp(-coupling))

MESH = pl.DeviceIdType.MESH


def circulant(rate):
    k = np.arange(L)
    spectrum = np.exp(rate * np.cos(2.0 * np.pi * k / L))
    differ = k[:, None] - k[None, :]
    waves = np.cos(2.0 * np.pi * (differ[:, :, None] * k) / L)
    return (waves * spectrum).sum(-1) / L


def high_low(matrix):
    matrix = matrix.astype(np.float32)
    high = matrix.astype(jnp.bfloat16)
    low = (matrix - high.astype(np.float32)).astype(jnp.bfloat16)
    return high, low


def as_left(matrix):
    high, low = high_low(matrix)
    return np.concatenate([high, low, high], axis=1)


def as_right(matrix, columns):
    both = np.kron(np.eye(2), matrix)[:, columns]
    high, low = high_low(both)
    upper = np.concatenate([high, low], axis=1)
    lower = np.concatenate([high, np.zeros_like(low)], axis=1)
    return np.concatenate([upper, lower], axis=0)


def split(values):
    high = values.astype(jnp.bfloat16)
    low = (values - high.astype(jnp.float32)).astype(jnp.bfloat16)
    return high, low


def mix_rows(weights, values):
    high, low = split(values)
    stacked = jnp.concatenate([high, high, low], axis=0)
    return jnp.dot(weights, stacked, preferred_element_type=jnp.float32)


def mix_lanes(values, weights):
    high, low = split(values)
    wide = jnp.concatenate([high, low], axis=1)
    both = jnp.dot(wide, weights, preferred_element_type=jnp.float32)
    return both[:, :128] + both[:, 128:]


def lane(shape):
    return lax.broadcasted_iota(jnp.int32, shape, len(shape) - 1)


def swap_lanes(first, second, width):
    keep = (lane(first.shape) // width) % 2 == 0
    return (
        jnp.where(keep, first, pltpu.roll(second, width, 1)),
        jnp.where(keep, pltpu.roll(first, 128 - width, 1), second),
    )


def swap_blocks(tiles):
    t0, t2 = swap_lanes(tiles[0], tiles[2], 64)
    t1, t3 = swap_lanes(tiles[1], tiles[3], 64)
    t0, t1 = swap_lanes(t0, t1, 32)
    t2, t3 = swap_lanes(t2, t3, 32)
    return [t0, t1, t2, t3]


def rows_of_tiles(tiles):
    return jnp.concatenate(swap_blocks(tiles), axis=0)


def tiles_of_rows(rows):
    return swap_blocks([rows[k * ROWS : (k + 1) * ROWS] for k in range(BLOCKS)])


def beside(tiles):
    return jnp.concatenate(tiles, axis=1)


def mix_tiles(weights, tiles):
    mixed = [mix_rows(weights, beside(tiles[k : k + 2])) for k in range(0, len(tiles), 2)]
    return [half for pair in mixed for half in (pair[:, :128], pair[:, 128:])]


def kernel(
    green_ref, field_hbm, left_hbm, last_hbm, lanes_hbm, lanes_last_hbm, right_hbm, out_ref,
    field_ref, left_ref, last_ref, lanes_ref, lanes_last_ref, right_ref, held, gain, turn, own_scale, scale_x, scale_y,
    outgoing, arrived, lines, returning, landed,
    small_sems, load_sem, send_sem, recv_sems, back_send_sem, back_recv_sems,
):
    me = lax.axis_index("cols")
    barrier = pltpu.get_barrier_semaphore()

    def greet(k, carry):
        pl.semaphore_signal(
            barrier, inc=1, device_id={"cols": lax.rem(me + k, PEERS)}, device_id_type=MESH
        )
        return carry

    lax.fori_loop(1, PEERS, greet, 0)

    loads = [
        pltpu.make_async_copy(
            green_ref.at[:, pl.ds(t * 128, 128)],
            held.at[pl.ds(t * PITCH_IN, L), :],
            load_sem,
        )
        for t in range(TILES)
    ]
    smalls = [
        pltpu.make_async_copy(source, target, small_sems.at[k])
        for k, (source, target) in enumerate(
            [
                (field_hbm, field_ref),
                (left_hbm, left_ref),
                (lanes_hbm, lanes_ref),
                (last_hbm, last_ref),
                (lanes_last_hbm, lanes_last_ref),
                (right_hbm, right_ref),
            ]
        )
    ]
    smalls[0].start()
    for load in loads:
        load.start()
    for small in smalls[1:]:
        small.start()

    smalls[0].wait()
    low_half = lane((TILES, 128)) < 64
    for moment in range(SLICES):
        bits = field_ref[moment * TILES : (moment + 1) * TILES, :].astype(jnp.float32)
        turned = pltpu.roll(bits, 64, 1)
        even = jnp.where(low_half, bits, turned)
        odd = jnp.where(low_half, turned, bits)
        gain[moment * L : moment * L + TILES, :] = jnp.where(even > 0.5, UP, DOWN)
        gain[moment * L + TILES : (moment + 1) * L, :] = jnp.where(odd > 0.5, UP, DOWN)
        turn[pl.ds(moment * L, TILES, stride=2), :] = bits
        turn[pl.ds(moment * L + 1, TILES, stride=2), :] = turned
    mine = jnp.broadcast_to(turn[pl.ds(me, 1), :], (ROWS, 128))
    site = lane((ROWS, 128))
    spot_row = lax.broadcasted_iota(jnp.int32, (ROWS, 128), 0)
    own_bits = jnp.zeros((ROWS, 128), jnp.float32)
    for block in range(BLOCKS):
        picked = jnp.where(site == spot_row + block * ROWS, mine, 0.0)
        own_bits = jnp.where(site // 32 == block, jnp.sum(picked, axis=1, keepdims=True), own_bits)
    own_scale[...] = jnp.where(own_bits > 0.5, DOWN, UP)

    for small in smalls[1:]:
        small.wait()
    pltpu.make_async_copy(arrived, arrived, load_sem).wait()

    def send_out(half, start, count):
        def one(k, carry):
            peer = lax.rem(me + k, PEERS)
            pltpu.make_async_remote_copy(
                src_ref=outgoing.at[pl.ds(pl.multiple_of((half * PEERS + peer) * PITCH_OUT + start, 8), count), :],
                dst_ref=arrived.at[half * PEERS + me, pl.ds(pl.multiple_of(start, 8), count), :],
                send_sem=send_sem,
                recv_sem=recv_sems.at[half * 2 + lax.rem(peer // BLOCKS + ROWS - me // BLOCKS, ROWS) // GROUP],
                device_id={"cols": peer},
                device_id_type=MESH,
            ).start()
            return carry

        lax.fori_loop(1, PEERS, one, 0)

    def left_step(step, carry):
        base = step * PER_STEP
        tiles = []
        for k in range(PER_STEP):
            for upper in range(2):
                row = base + k + upper * 2 * ROWS
                pair = swap_lanes(
                    held[pl.ds(row, TILES, stride=PITCH_IN), :],
                    held[pl.ds(row + ROWS, TILES, stride=PITCH_IN), :],
                    64,
                )
                tiles.append(jnp.concatenate(pair, axis=0))
        for moment in range(SLICES):
            ends = moment == SLICES - 1
            scale = gain[moment * L : (moment + 1) * L, :]
            tiles = mix_tiles((last_ref if ends else left_ref)[...], [tile * scale for tile in tiles])
            weights = (lanes_last_ref if ends else lanes_ref)[...]
            stack = mix_lanes(jnp.concatenate(tiles, axis=0), weights)
            tiles = [stack[k * L : (k + 1) * L] for k in range(len(tiles))]
        for k in range(PER_STEP):
            row = own_scale[pl.ds(base + k, 1), :]
            for half, tile in enumerate(swap_lanes(tiles[2 * k], tiles[2 * k + 1], 64)):
                outgoing[pl.ds(half * PEERS * PITCH_OUT + base + k, L, stride=PITCH_OUT), :] = tile * row

        @pl.when(step == 0)
        def _():
            pl.semaphore_wait(barrier, PEERS - 1)

        send_out(0, base, PER_STEP)
        return carry

    lax.fori_loop(0, STEPS, left_step, 0)
    send_out(1, 0, ROWS)

    for half in range(HALVES):
        arrived[half * PEERS + me] = outgoing[pl.ds(pl.multiple_of((half * PEERS + me) * PITCH_OUT, 8), ROWS), :]

    square = jnp.concatenate([turn[2 * L : 3 * L, :], jnp.zeros((L, 128), jnp.float32)], axis=0)
    turn[3 * L : 4 * L, :] = square.T[:L, :]

    def spread(k, carry):
        block = lane((128, 128)) // 32
        from_row = lax.broadcasted_iota(jnp.int32, (128, 128), 0)
        hot_y = (from_row == block * ROWS + k).astype(jnp.bfloat16)
        hot_x = (from_row == block + k * BLOCKS).astype(jnp.bfloat16)
        wide_y = jnp.dot(turn[L : 2 * L, :].astype(jnp.bfloat16), hot_y, preferred_element_type=jnp.float32)
        wide_x = jnp.dot(turn[3 * L : 4 * L, :].astype(jnp.bfloat16), hot_x, preferred_element_type=jnp.float32)
        scale_x[k] = jnp.where(wide_y > 0.5, DOWN, UP)
        scale_y[k] = jnp.where(wide_x > 0.5, DOWN, UP)
        return carry

    lax.fori_loop(0, ROWS, spread, 0)

    def wait_blocks(sem, buffer, count):
        blocks = buffer.at[pl.ds(0, count)]
        pltpu.make_async_remote_copy(
            src_ref=blocks,
            dst_ref=blocks,
            send_sem=send_sem,
            recv_sem=sem,
            device_id={"cols": lax.rem(me + 1, PEERS)},
            device_id_type=MESH,
        ).wait_recv()

    def wait_group(sem, buffer, step, count, own):
        @pl.when(step == 0)
        def _():
            wait_blocks(sem, buffer, count - own)

        @pl.when(step != 0)
        def _():
            wait_blocks(sem, buffer, count)

    group = GROUP

    def right_half(half, carry):
        weights = right_ref[...]

        def store_lines(spots, tiles):
            for spot, rows in zip(spots, tiles):
                for k, tile in enumerate(tiles_of_rows(rows)):
                    lines[pl.ds(spot * BLOCKS + k, ROWS, stride=PITCH_X), :] = tile

        def by_lines(step, carry):
            spots = [lax.rem(me // BLOCKS + 2 * ROWS - step * group - k, ROWS) for k in range(group)]
            wait_group(recv_sems.at[half * 2 + step], arrived, step, group * BLOCKS, 1)
            tiles = [
                rows_of_tiles([arrived[half * PEERS + spot * BLOCKS + k] for k in range(BLOCKS)]) for spot in spots
            ]
            store_lines(spots, mix_tiles(weights, tiles))
            return carry

        lax.fori_loop(0, ROWS // group, by_lines, 0)

        def across(step, carry):
            spots = [step * group + k for k in range(group)]
            tiles = [lines[pl.ds(pl.multiple_of(spot * PITCH_X, 8), L), :] for spot in spots]
            tiles = mix_tiles(weights, tiles)
            tiles = mix_tiles(weights, [tile * scale_x[spot] for spot, tile in zip(spots, tiles)])
            for spot, tile in zip(spots, tiles):
                lines[pl.ds(pl.multiple_of(spot * PITCH_X, 8), L), :] = tile
            return carry

        lax.fori_loop(0, ROWS // group, across, 0)

        def along(step, carry):
            spots = [step * group + k for k in range(group)]
            tiles = [
                rows_of_tiles([lines[pl.ds(spot * BLOCKS + k, ROWS, stride=PITCH_X), :] for k in range(BLOCKS)])
                for spot in spots
            ]
            tiles = mix_tiles(weights, tiles)
            tiles = mix_tiles(weights, [tile * scale_y[spot] for spot, tile in zip(spots, tiles)])
            store_lines(spots, tiles)
            return carry

        lax.fori_loop(0, ROWS // group, along, 0)

        def finish(step, carry):
            spots = [step * group + k for k in range(group)]
            tiles = [lines[pl.ds(pl.multiple_of(spot * PITCH_X, 8), L), :] for spot in spots]
            for spot, tile in zip(spots, mix_tiles(weights, tiles)):
                returning[pl.ds(half * PEERS * PITCH_OUT + spot, L, stride=PITCH_OUT), :] = tile
            return carry

        lax.fori_loop(0, ROWS // group, finish, 0)

        def send_back(k, carry):
            peer = lax.rem(me + k, PEERS)
            pltpu.make_async_remote_copy(
                src_ref=returning.at[pl.ds(pl.multiple_of((half * PEERS + peer) * PITCH_OUT, 8), ROWS), :],
                dst_ref=landed.at[half * PEERS + me],
                send_sem=back_send_sem,
                recv_sem=back_recv_sems.at[lax.rem(peer // 2 + TILES - me // 2, TILES) // MERGED],
                device_id={"cols": peer},
                device_id_type=MESH,
            ).start()
            return carry

        lax.fori_loop(1, PEERS, send_back, 0)
        landed[half * PEERS + me] = returning[pl.ds(pl.multiple_of((half * PEERS + me) * PITCH_OUT, 8), ROWS), :]
        return carry

    lax.fori_loop(0, HALVES, right_half, 0)

    def merge(step, carry):
        spots = [lax.rem(me // 2 + 2 * TILES - step * MERGED - k, TILES) for k in range(MERGED)]
        wait_group(back_recv_sems.at[step], landed, step, MERGED * 2 * HALVES, HALVES)
        for spot in spots:
            tiles = [landed[half * PEERS + 2 * spot + q] for q in range(2) for half in range(HALVES)]
            columns = pl.ds(pl.multiple_of(spot * 128, 128), 128)
            for k, tile in enumerate(swap_blocks(tiles)):
                out_ref[k * ROWS : (k + 1) * ROWS, columns] = tile
        return carry

    lax.fori_loop(0, TILES // MERGED, merge, 0)

    for buffer, sem in ((arrived, send_sem), (landed, back_send_sem)):
        everything = buffer.at[pl.ds(0, HALVES * (PEERS - 1))]
        pltpu.make_async_remote_copy(
            src_ref=everything,
            dst_ref=everything,
            send_sem=sem,
            recv_sem=recv_sems.at[0],
            device_id={"cols": lax.rem(me + 1, PEERS)},
            device_id_type=MESH,
        ).wait_send()


def shards(green_by_column, field):
    green = green_by_column.reshape(L, SITES)
    bits = field.reshape(SLICES * TILES, 128)
    order = np.concatenate([np.arange(0, L, 2), np.arange(1, L, 2)])
    columns = np.arange(128).reshape(2, HALVES, 32).transpose(1, 0, 2).reshape(128)
    forward = circulant(hop_rate)
    inverse = circulant(-hop_rate)
    left = jnp.asarray(as_left(forward[np.ix_(order, order)]))
    last = jnp.asarray(as_left(forward[:, order]))
    lanes = jnp.asarray(as_right(forward, np.arange(128)))
    lanes_last = jnp.asarray(as_right(forward, columns))
    right = jnp.asarray(as_left(inverse))
    vmem = pl.BlockSpec(memory_space=pltpu.VMEM)
    wrapped = pl.pallas_call(
        kernel,
        out_shape=pltpu.VMEM((L, SITES), jnp.float32),
        in_specs=[pl.BlockSpec(memory_space=pl.ANY)] * 7,
        out_specs=vmem,
        scratch_shapes=[
            pltpu.VMEM((SLICES * TILES, 128), jnp.int32),
            pltpu.VMEM(left.shape, jnp.bfloat16),
            pltpu.VMEM(last.shape, jnp.bfloat16),
            pltpu.VMEM(lanes.shape, jnp.bfloat16),
            pltpu.VMEM(lanes_last.shape, jnp.bfloat16),
            pltpu.VMEM(right.shape, jnp.bfloat16),
            pltpu.VMEM((TILES * PITCH_IN, 128), jnp.float32),
            pltpu.VMEM((SLICES * L, 128), jnp.float32),
            pltpu.VMEM((4 * L, 128), jnp.float32),
            pltpu.VMEM((ROWS, 128), jnp.float32),
            pltpu.VMEM((ROWS, L, 128), jnp.float32),
            pltpu.VMEM((ROWS, L, 128), jnp.float32),
            pltpu.VMEM((HALVES * PEERS * PITCH_OUT, 128), jnp.float32),
            pltpu.VMEM((HALVES * PEERS, ROWS, 128), jnp.float32),
            pltpu.VMEM((ROWS * PITCH_X, 128), jnp.float32),
            pltpu.VMEM((HALVES * PEERS * PITCH_OUT, 128), jnp.float32),
            pltpu.VMEM((HALVES * PEERS, ROWS, 128), jnp.float32),
            pltpu.SemaphoreType.DMA((6,)),
            pltpu.SemaphoreType.DMA,
            pltpu.SemaphoreType.DMA,
            pltpu.SemaphoreType.DMA((HALVES * ROWS // GROUP,)),
            pltpu.SemaphoreType.DMA,
            pltpu.SemaphoreType.DMA((TILES // MERGED,)),
        ],
        compiler_params=pltpu.CompilerParams(collective_id=0, has_side_effects=True),
    )(green, bits, left, last, lanes, lanes_last, right)
    return wrapped.reshape(1, L, SITES)


def solution(mesh):
    return jax.shard_map(
        shards,
        mesh=mesh,
        in_specs=(P("walk", "cols", None), P("walk", None, None)),
        out_specs=P("walk", "cols", None),
        check_vma=False,
    )
```

```python
import jax
import jax.numpy as jnp
import numpy as np
from jax import lax
from jax.experimental import pallas as pl
from jax.experimental.pallas import tpu as pltpu
from jax.sharding import PartitionSpec as P

L = 64
SITES = L * L
SLICES = 3
PEERS = 64
TILES = SITES // 128
BLOCKS = 4
ROWS = L // BLOCKS
HALVES = 2
STEPS = 2
PER_STEP = ROWS // STEPS
GROUP = 8
MERGED = 4
PITCH_IN = 72
PITCH_OUT = 24
PITCH_X = 72

hop_rate = 0.6
coupling = 0.65373
UP = float(np.exp(coupling))
DOWN = float(np.exp(-coupling))

MESH = pl.DeviceIdType.MESH


def circulant(rate):
    k = np.arange(L)
    spectrum = np.exp(rate * np.cos(2.0 * np.pi * k / L))
    differ = k[:, None] - k[None, :]
    waves = np.cos(2.0 * np.pi * (differ[:, :, None] * k) / L)
    return (waves * spectrum).sum(-1) / L


def high_low(matrix):
    matrix = matrix.astype(np.float32)
    high = matrix.astype(jnp.bfloat16)
    low = (matrix - high.astype(np.float32)).astype(jnp.bfloat16)
    return high, low


def as_left(matrix):
    high, low = high_low(matrix)
    return np.concatenate([high, low, high], axis=1)


def as_right(matrix, columns):
    both = np.kron(np.eye(2), matrix)[:, columns]
    high, low = high_low(both)
    upper = np.concatenate([high, low], axis=1)
    lower = np.concatenate([high, np.zeros_like(low)], axis=1)
    return np.concatenate([upper, lower], axis=0)


def split(values):
    high = values.astype(jnp.bfloat16)
    low = (values - high.astype(jnp.float32)).astype(jnp.bfloat16)
    return high, low


def mix_rows(weights, values):
    high, low = split(values)
    stacked = jnp.concatenate([high, high, low], axis=0)
    return jnp.dot(weights, stacked, preferred_element_type=jnp.float32)


def mix_lanes(values, weights):
    high, low = split(values)
    wide = jnp.concatenate([high, low], axis=1)
    both = jnp.dot(wide, weights, preferred_element_type=jnp.float32)
    return both[:, :128] + both[:, 128:]


def lane(shape):
    return lax.broadcasted_iota(jnp.int32, shape, len(shape) - 1)


def swap_lanes(first, second, width):
    keep = (lane(first.shape) // width) % 2 == 0
    return (
        jnp.where(keep, first, pltpu.roll(second, width, 1)),
        jnp.where(keep, pltpu.roll(first, 128 - width, 1), second),
    )


def swap_blocks(tiles):
    t0, t2 = swap_lanes(tiles[0], tiles[2], 64)
    t1, t3 = swap_lanes(tiles[1], tiles[3], 64)
    t0, t1 = swap_lanes(t0, t1, 32)
    t2, t3 = swap_lanes(t2, t3, 32)
    return [t0, t1, t2, t3]


def rows_of_tiles(tiles):
    return jnp.concatenate(swap_blocks(tiles), axis=0)


def tiles_of_rows(rows):
    return swap_blocks([rows[k * ROWS : (k + 1) * ROWS] for k in range(BLOCKS)])


def beside(tiles):
    return jnp.concatenate(tiles, axis=1)


def mix_tiles(weights, tiles):
    mixed = [mix_rows(weights, beside(tiles[k : k + 2])) for k in range(0, len(tiles), 2)]
    return [half for pair in mixed for half in (pair[:, :128], pair[:, 128:])]


def kernel(
    green_ref, field_hbm, left_hbm, last_hbm, lanes_hbm, lanes_last_hbm, right_hbm, out_ref,
    field_ref, left_ref, last_ref, lanes_ref, lanes_last_ref, right_ref, held, gain, turn, own_scale, scale_x, scale_y,
    outgoing, arrived, lines, returning, landed,
    small_sems, load_sem, send_sem, recv_sems, back_send_sem, back_recv_sems,
):
    me = lax.axis_index("cols")
    barrier = pltpu.get_barrier_semaphore()

    def greet(k, carry):
        pl.semaphore_signal(
            barrier, inc=1, device_id={"cols": lax.rem(me + k, PEERS)}, device_id_type=MESH
        )
        return carry

    lax.fori_loop(1, PEERS, greet, 0)

    loads = [
        pltpu.make_async_copy(
            green_ref.at[:, pl.ds(t * 128, 128)],
            held.at[pl.ds(t * PITCH_IN, L), :],
            load_sem,
        )
        for t in range(TILES)
    ]
    smalls = [
        pltpu.make_async_copy(source, target, small_sems.at[k])
        for k, (source, target) in enumerate(
            [
                (field_hbm, field_ref),
                (left_hbm, left_ref),
                (lanes_hbm, lanes_ref),
                (last_hbm, last_ref),
                (lanes_last_hbm, lanes_last_ref),
                (right_hbm, right_ref),
            ]
        )
    ]
    smalls[0].start()
    for load in loads:
        load.start()
    for small in smalls[1:]:
        small.start()

    smalls[0].wait()
    low_half = lane((TILES, 128)) < 64
    for moment in range(SLICES):
        bits = field_ref[moment * TILES : (moment + 1) * TILES, :].astype(jnp.float32)
        turned = pltpu.roll(bits, 64, 1)
        even = jnp.where(low_half, bits, turned)
        odd = jnp.where(low_half, turned, bits)
        gain[moment * L : moment * L + TILES, :] = jnp.where(even > 0.5, UP, DOWN)
        gain[moment * L + TILES : (moment + 1) * L, :] = jnp.where(odd > 0.5, UP, DOWN)
        turn[pl.ds(moment * L, TILES, stride=2), :] = bits
        turn[pl.ds(moment * L + 1, TILES, stride=2), :] = turned
    mine = jnp.broadcast_to(turn[pl.ds(me, 1), :], (ROWS, 128))
    site = lane((ROWS, 128))
    spot_row = lax.broadcasted_iota(jnp.int32, (ROWS, 128), 0)
    own_bits = jnp.zeros((ROWS, 128), jnp.float32)
    for block in range(BLOCKS):
        picked = jnp.where(site == spot_row + block * ROWS, mine, 0.0)
        own_bits = jnp.where(site // 32 == block, jnp.sum(picked, axis=1, keepdims=True), own_bits)
    own_scale[...] = jnp.where(own_bits > 0.5, DOWN, UP)

    for small in smalls[1:]:
        small.wait()
    pltpu.make_async_copy(arrived, arrived, load_sem).wait()

    def send_out(half, start, count):
        def one(k, carry):
            peer = lax.rem(me + k, PEERS)
            pltpu.make_async_remote_copy(
                src_ref=outgoing.at[pl.ds(pl.multiple_of((half * PEERS + peer) * PITCH_OUT + start, 8), count), :],
                dst_ref=arrived.at[half * PEERS + me, pl.ds(pl.multiple_of(start, 8), count), :],
                send_sem=send_sem,
                recv_sem=recv_sems.at[half * 2 + lax.rem(peer // BLOCKS + ROWS - me // BLOCKS, ROWS) // GROUP],
                device_id={"cols": peer},
                device_id_type=MESH,
            ).start()
            return carry

        lax.fori_loop(1, PEERS, one, 0)

    def left_step(step, carry):
        base = step * PER_STEP
        tiles = []
        for k in range(PER_STEP):
            for upper in range(2):
                row = base + k + upper * 2 * ROWS
                pair = swap_lanes(
                    held[pl.ds(row, TILES, stride=PITCH_IN), :],
                    held[pl.ds(row + ROWS, TILES, stride=PITCH_IN), :],
                    64,
                )
                tiles.append(jnp.concatenate(pair, axis=0))
        for moment in range(SLICES):
            ends = moment == SLICES - 1
            scale = gain[moment * L : (moment + 1) * L, :]
            tiles = mix_tiles((last_ref if ends else left_ref)[...], [tile * scale for tile in tiles])
            weights = (lanes_last_ref if ends else lanes_ref)[...]
            stack = mix_lanes(jnp.concatenate(tiles, axis=0), weights)
            tiles = [stack[k * L : (k + 1) * L] for k in range(len(tiles))]
        for k in range(PER_STEP):
            row = own_scale[pl.ds(base + k, 1), :]
            for half, tile in enumerate(swap_lanes(tiles[2 * k], tiles[2 * k + 1], 64)):
                outgoing[pl.ds(half * PEERS * PITCH_OUT + base + k, L, stride=PITCH_OUT), :] = tile * row

        @pl.when(step == 0)
        def _():
            pl.semaphore_wait(barrier, PEERS - 1)

        send_out(0, base, PER_STEP)
        return carry

    lax.fori_loop(0, STEPS, left_step, 0)
    send_out(1, 0, ROWS)

    for half in range(HALVES):
        arrived[half * PEERS + me] = outgoing[pl.ds(pl.multiple_of((half * PEERS + me) * PITCH_OUT, 8), ROWS), :]

    square = jnp.concatenate([turn[2 * L : 3 * L, :], jnp.zeros((L, 128), jnp.float32)], axis=0)
    turn[3 * L : 4 * L, :] = square.T[:L, :]

    def spread(k, carry):
        block = lane((128, 128)) // 32
        from_row = lax.broadcasted_iota(jnp.int32, (128, 128), 0)
        hot_y = (from_row == block * ROWS + k).astype(jnp.bfloat16)
        hot_x = (from_row == block + k * BLOCKS).astype(jnp.bfloat16)
        wide_y = jnp.dot(turn[L : 2 * L, :].astype(jnp.bfloat16), hot_y, preferred_element_type=jnp.float32)
        wide_x = jnp.dot(turn[3 * L : 4 * L, :].astype(jnp.bfloat16), hot_x, preferred_element_type=jnp.float32)
        scale_x[k] = jnp.where(wide_y > 0.5, DOWN, UP)
        scale_y[k] = jnp.where(wide_x > 0.5, DOWN, UP)
        return carry

    lax.fori_loop(0, ROWS, spread, 0)

    def wait_blocks(sem, buffer, count):
        blocks = buffer.at[pl.ds(0, count)]
        pltpu.make_async_remote_copy(
            src_ref=blocks,
            dst_ref=blocks,
            send_sem=send_sem,
            recv_sem=sem,
            device_id={"cols": lax.rem(me + 1, PEERS)},
            device_id_type=MESH,
        ).wait_recv()

    def wait_group(sem, buffer, step, count, own):
        @pl.when(step == 0)
        def _():
            wait_blocks(sem, buffer, count - own)

        @pl.when(step != 0)
        def _():
            wait_blocks(sem, buffer, count)

    group = GROUP

    def right_half(half, carry):
        weights = right_ref[...]

        def store_lines(spots, tiles):
            for spot, rows in zip(spots, tiles):
                for k, tile in enumerate(tiles_of_rows(rows)):
                    lines[pl.ds(spot * BLOCKS + k, ROWS, stride=PITCH_X), :] = tile

        def by_lines(step, carry):
            spots = [lax.rem(me // BLOCKS + 2 * ROWS - step * group - k, ROWS) for k in range(group)]
            wait_group(recv_sems.at[half * 2 + step], arrived, step, group * BLOCKS, 1)
            tiles = [
                rows_of_tiles([arrived[half * PEERS + spot * BLOCKS + k] for k in range(BLOCKS)]) for spot in spots
            ]
            store_lines(spots, mix_tiles(weights, tiles))
            return carry

        lax.fori_loop(0, ROWS // group, by_lines, 0)

        def across(step, carry):
            spots = [step * group + k for k in range(group)]
            tiles = [lines[pl.ds(pl.multiple_of(spot * PITCH_X, 8), L), :] for spot in spots]
            tiles = mix_tiles(weights, tiles)
            tiles = mix_tiles(weights, [tile * scale_x[spot] for spot, tile in zip(spots, tiles)])
            for spot, tile in zip(spots, tiles):
                lines[pl.ds(pl.multiple_of(spot * PITCH_X, 8), L), :] = tile
            return carry

        lax.fori_loop(0, ROWS // group, across, 0)

        def along(step, carry):
            spots = [step * group + k for k in range(group)]
            tiles = [
                rows_of_tiles([lines[pl.ds(spot * BLOCKS + k, ROWS, stride=PITCH_X), :] for k in range(BLOCKS)])
                for spot in spots
            ]
            tiles = mix_tiles(weights, tiles)
            tiles = mix_tiles(weights, [tile * scale_y[spot] for spot, tile in zip(spots, tiles)])
            store_lines(spots, tiles)
            return carry

        lax.fori_loop(0, ROWS // group, along, 0)

        def finish(step, carry):
            spots = [step * group + k for k in range(group)]
            tiles = [lines[pl.ds(pl.multiple_of(spot * PITCH_X, 8), L), :] for spot in spots]
            for spot, tile in zip(spots, mix_tiles(weights, tiles)):
                returning[pl.ds(half * PEERS * PITCH_OUT + spot, L, stride=PITCH_OUT), :] = tile
            return carry

        lax.fori_loop(0, ROWS // group, finish, 0)

        def send_back(k, carry):
            peer = lax.rem(me + k, PEERS)
            pltpu.make_async_remote_copy(
                src_ref=returning.at[pl.ds(pl.multiple_of((half * PEERS + peer) * PITCH_OUT, 8), ROWS), :],
                dst_ref=landed.at[half * PEERS + me],
                send_sem=back_send_sem,
                recv_sem=back_recv_sems.at[lax.rem(peer // 2 + TILES - me // 2, TILES) // MERGED],
                device_id={"cols": peer},
                device_id_type=MESH,
            ).start()
            return carry

        lax.fori_loop(1, PEERS, send_back, 0)
        landed[half * PEERS + me] = returning[pl.ds(pl.multiple_of((half * PEERS + me) * PITCH_OUT, 8), ROWS), :]
        return carry

    lax.fori_loop(0, HALVES, right_half, 0)

    def merge(step, carry):
        spots = [lax.rem(me // 2 + 2 * TILES - step * MERGED - k, TILES) for k in range(MERGED)]
        wait_group(back_recv_sems.at[step], landed, step, MERGED * 2 * HALVES, HALVES)
        for spot in spots:
            tiles = [landed[half * PEERS + 2 * spot + q] for q in range(2) for half in range(HALVES)]
            columns = pl.ds(pl.multiple_of(spot * 128, 128), 128)
            for k, tile in enumerate(swap_blocks(tiles)):
                out_ref[k * ROWS : (k + 1) * ROWS, columns] = tile
        return carry

    lax.fori_loop(0, TILES // MERGED, merge, 0)

    for buffer, sem in ((arrived, send_sem), (landed, back_send_sem)):
        everything = buffer.at[pl.ds(0, HALVES * (PEERS - 1))]
        pltpu.make_async_remote_copy(
            src_ref=everything,
            dst_ref=everything,
            send_sem=sem,
            recv_sem=recv_sems.at[0],
            device_id={"cols": lax.rem(me + 1, PEERS)},
            device_id_type=MESH,
        ).wait_send()


def shards(green_by_column, field):
    green = green_by_column.reshape(L, SITES)
    bits = field.reshape(SLICES * TILES, 128)
    order = np.concatenate([np.arange(0, L, 2), np.arange(1, L, 2)])
    columns = np.arange(128).reshape(2, HALVES, 32).transpose(1, 0, 2).reshape(128)
    forward = circulant(hop_rate)
    inverse = circulant(-hop_rate)
    left = jnp.asarray(as_left(forward[np.ix_(order, order)]))
    last = jnp.asarray(as_left(forward[:, order]))
    lanes = jnp.asarray(as_right(forward, np.arange(128)))
    lanes_last = jnp.asarray(as_right(forward, columns))
    right = jnp.asarray(as_left(inverse))
    vmem = pl.BlockSpec(memory_space=pltpu.VMEM)
    wrapped = pl.pallas_call(
        kernel,
        out_shape=pltpu.VMEM((L, SITES), jnp.float32),
        in_specs=[pl.BlockSpec(memory_space=pl.ANY)] * 7,
        out_specs=vmem,
        scratch_shapes=[
            pltpu.VMEM((SLICES * TILES, 128), jnp.int32),
            pltpu.VMEM(left.shape, jnp.bfloat16),
            pltpu.VMEM(last.shape, jnp.bfloat16),
            pltpu.VMEM(lanes.shape, jnp.bfloat16),
            pltpu.VMEM(lanes_last.shape, jnp.bfloat16),
            pltpu.VMEM(right.shape, jnp.bfloat16),
            pltpu.VMEM(((TILES + 1) * PITCH_IN, 128), jnp.float32),
            pltpu.VMEM((SLICES * L, 128), jnp.float32),
            pltpu.VMEM((4 * L, 128), jnp.float32),
            pltpu.VMEM((ROWS, 128), jnp.float32),
            pltpu.VMEM((ROWS, L, 128), jnp.float32),
            pltpu.VMEM((ROWS, L, 128), jnp.float32),
            pltpu.VMEM(((HALVES * PEERS + 1) * PITCH_OUT, 128), jnp.float32),
            pltpu.VMEM((HALVES * PEERS, ROWS, 128), jnp.float32),
            pltpu.VMEM(((ROWS + 1) * PITCH_X, 128), jnp.float32),
            pltpu.VMEM(((HALVES * PEERS + 1) * PITCH_OUT, 128), jnp.float32),
            pltpu.VMEM((HALVES * PEERS, ROWS, 128), jnp.float32),
            pltpu.SemaphoreType.DMA((6,)),
            pltpu.SemaphoreType.DMA,
            pltpu.SemaphoreType.DMA,
            pltpu.SemaphoreType.DMA((HALVES * ROWS // GROUP,)),
            pltpu.SemaphoreType.DMA,
            pltpu.SemaphoreType.DMA((TILES // MERGED,)),
        ],
        compiler_params=pltpu.CompilerParams(collective_id=0, has_side_effects=True),
    )(green, bits, left, last, lanes, lanes_last, right)
    return wrapped.reshape(1, L, SITES)


def solution(mesh):
    return jax.shard_map(
        shards,
        mesh=mesh,
        in_specs=(P("walk", "cols", None), P("walk", None, None)),
        out_specs=P("walk", "cols", None),
        check_vma=False,
    )
```

```python
import jax
import jax.numpy as jnp
import numpy as np
from jax import lax
from jax.experimental import pallas as pl
from jax.experimental.pallas import tpu as pltpu
from jax.sharding import PartitionSpec as P

L = 64
SITES = L * L
SLICES = 3
PEERS = 64
TILES = SITES // 128
BLOCKS = 4
ROWS = L // BLOCKS
HALVES = 2
STEPS = 2
PER_STEP = ROWS // STEPS
GROUP = 8
MERGED = 8
PITCH_IN = 72
PITCH_OUT = 24
PITCH_X = 72

hop_rate = 0.6
coupling = 0.65373
UP = float(np.exp(coupling))
DOWN = float(np.exp(-coupling))

MESH = pl.DeviceIdType.MESH


def circulant(rate):
    k = np.arange(L)
    spectrum = np.exp(rate * np.cos(2.0 * np.pi * k / L))
    differ = k[:, None] - k[None, :]
    waves = np.cos(2.0 * np.pi * (differ[:, :, None] * k) / L)
    return (waves * spectrum).sum(-1) / L


def high_low(matrix):
    matrix = matrix.astype(np.float32)
    high = matrix.astype(jnp.bfloat16)
    low = (matrix - high.astype(np.float32)).astype(jnp.bfloat16)
    return high, low


def as_left(matrix):
    high, low = high_low(matrix)
    return np.concatenate([high, low, high], axis=1)


def as_right(matrix, columns):
    both = np.kron(np.eye(2), matrix)[:, columns]
    high, low = high_low(both)
    upper = np.concatenate([high, low], axis=1)
    lower = np.concatenate([high, np.zeros_like(low)], axis=1)
    return np.concatenate([upper, lower], axis=0)


def split(values):
    high = values.astype(jnp.bfloat16)
    low = (values - high.astype(jnp.float32)).astype(jnp.bfloat16)
    return high, low


def mix_rows(weights, values):
    high, low = split(values)
    stacked = jnp.concatenate([high, high, low], axis=0)
    return jnp.dot(weights, stacked, preferred_element_type=jnp.float32)


def mix_lanes(values, weights):
    high, low = split(values)
    wide = jnp.concatenate([high, low], axis=1)
    both = jnp.dot(wide, weights, preferred_element_type=jnp.float32)
    return both[:, :128] + both[:, 128:]


def lane(shape):
    return lax.broadcasted_iota(jnp.int32, shape, len(shape) - 1)


def swap_lanes(first, second, width):
    keep = (lane(first.shape) // width) % 2 == 0
    return (
        jnp.where(keep, first, pltpu.roll(second, width, 1)),
        jnp.where(keep, pltpu.roll(first, 128 - width, 1), second),
    )


def swap_blocks(tiles):
    t0, t2 = swap_lanes(tiles[0], tiles[2], 64)
    t1, t3 = swap_lanes(tiles[1], tiles[3], 64)
    t0, t1 = swap_lanes(t0, t1, 32)
    t2, t3 = swap_lanes(t2, t3, 32)
    return [t0, t1, t2, t3]


def rows_of_tiles(tiles):
    return jnp.concatenate(swap_blocks(tiles), axis=0)


def tiles_of_rows(rows):
    return swap_blocks([rows[k * ROWS : (k + 1) * ROWS] for k in range(BLOCKS)])


def beside(tiles):
    return jnp.concatenate(tiles, axis=1)


def mix_tiles(weights, tiles):
    mixed = [mix_rows(weights, beside(tiles[k : k + 2])) for k in range(0, len(tiles), 2)]
    return [half for pair in mixed for half in (pair[:, :128], pair[:, 128:])]


def kernel(
    green_ref, field_hbm, narrow_hbm, wide_hbm, out_ref,
    field_ref, narrow_ref, wide_ref, held, gain, turn, own_scale, scale_x, scale_y,
    outgoing, arrived, lines, returning, landed,
    small_sems, load_sem, send_sem, recv_sems, back_send_sem, back_recv_sems,
):
    me = lax.axis_index("cols")
    barrier = pltpu.get_barrier_semaphore()
    left_ref, last_ref, right_ref = (narrow_ref.at[k * L : (k + 1) * L] for k in range(3))
    lanes_ref, lanes_last_ref = (wide_ref.at[k * 256 : (k + 1) * 256] for k in range(2))

    def greet(k, carry):
        pl.semaphore_signal(
            barrier, inc=1, device_id={"cols": lax.rem(me + k, PEERS)}, device_id_type=MESH
        )
        return carry

    lax.fori_loop(1, PEERS, greet, 0)

    loads = [
        pltpu.make_async_copy(
            green_ref.at[:, pl.ds(t * 128, 128)],
            held.at[pl.ds(t * PITCH_IN, L), :],
            load_sem,
        )
        for t in range(TILES)
    ]
    smalls = [
        pltpu.make_async_copy(source, target, small_sems.at[k])
        for k, (source, target) in enumerate(
            [
                (field_hbm, field_ref),
                (narrow_hbm, narrow_ref),
                (wide_hbm, wide_ref),
            ]
        )
    ]
    smalls[0].start()
    for load in loads:
        load.start()
    for small in smalls[1:]:
        small.start()

    smalls[0].wait()
    low_half = lane((TILES, 128)) < 64
    for moment in range(SLICES):
        bits = field_ref[moment * TILES : (moment + 1) * TILES, :].astype(jnp.float32)
        turned = pltpu.roll(bits, 64, 1)
        even = jnp.where(low_half, bits, turned)
        odd = jnp.where(low_half, turned, bits)
        gain[moment * L : moment * L + TILES, :] = jnp.where(even > 0.5, UP, DOWN)
        gain[moment * L + TILES : (moment + 1) * L, :] = jnp.where(odd > 0.5, UP, DOWN)
        turn[pl.ds(moment * L, TILES, stride=2), :] = bits
        turn[pl.ds(moment * L + 1, TILES, stride=2), :] = turned
    mine = jnp.broadcast_to(turn[pl.ds(me, 1), :], (ROWS, 128))
    site = lane((ROWS, 128))
    spot_row = lax.broadcasted_iota(jnp.int32, (ROWS, 128), 0)
    own_bits = jnp.zeros((ROWS, 128), jnp.float32)
    for block in range(BLOCKS):
        picked = jnp.where(site == spot_row + block * ROWS, mine, 0.0)
        own_bits = jnp.where(site // 32 == block, jnp.sum(picked, axis=1, keepdims=True), own_bits)
    own_scale[...] = jnp.where(own_bits > 0.5, DOWN, UP)

    for small in smalls[1:]:
        small.wait()
    pltpu.make_async_copy(arrived, arrived, load_sem).wait()

    def send_out(half, start, count):
        def one(k, carry):
            peer = lax.rem(me + k, PEERS)
            pltpu.make_async_remote_copy(
                src_ref=outgoing.at[pl.ds(pl.multiple_of((half * PEERS + peer) * PITCH_OUT + start, 8), count), :],
                dst_ref=arrived.at[half * PEERS + me, pl.ds(pl.multiple_of(start, 8), count), :],
                send_sem=send_sem,
                recv_sem=recv_sems.at[half * 2 + lax.rem(peer // BLOCKS + ROWS - me // BLOCKS, ROWS) // GROUP],
                device_id={"cols": peer},
                device_id_type=MESH,
            ).start()
            return carry

        lax.fori_loop(1, PEERS, one, 0)

    def left_step(step, carry):
        base = step * PER_STEP
        tiles = []
        for k in range(PER_STEP):
            for upper in range(2):
                row = base + k + upper * 2 * ROWS
                pair = swap_lanes(
                    held[pl.ds(row, TILES, stride=PITCH_IN), :],
                    held[pl.ds(row + ROWS, TILES, stride=PITCH_IN), :],
                    64,
                )
                tiles.append(jnp.concatenate(pair, axis=0))
        for moment in range(SLICES):
            ends = moment == SLICES - 1
            scale = gain[moment * L : (moment + 1) * L, :]
            tiles = mix_tiles((last_ref if ends else left_ref)[...], [tile * scale for tile in tiles])
            weights = (lanes_last_ref if ends else lanes_ref)[...]
            stack = mix_lanes(jnp.concatenate(tiles, axis=0), weights)
            tiles = [stack[k * L : (k + 1) * L] for k in range(len(tiles))]
        for k in range(PER_STEP):
            row = own_scale[pl.ds(base + k, 1), :]
            for half, tile in enumerate(swap_lanes(tiles[2 * k], tiles[2 * k + 1], 64)):
                outgoing[pl.ds(half * PEERS * PITCH_OUT + base + k, L, stride=PITCH_OUT), :] = tile * row

        @pl.when(step == 0)
        def _():
            pl.semaphore_wait(barrier, PEERS - 1)

        send_out(0, base, PER_STEP)
        return carry

    lax.fori_loop(0, STEPS, left_step, 0)
    send_out(1, 0, ROWS)

    for half in range(HALVES):
        arrived[half * PEERS + me] = outgoing[pl.ds(pl.multiple_of((half * PEERS + me) * PITCH_OUT, 8), ROWS), :]

    square = jnp.concatenate([turn[2 * L : 3 * L, :], jnp.zeros((L, 128), jnp.float32)], axis=0)
    turn[3 * L : 4 * L, :] = square.T[:L, :]

    def spread(k, carry):
        block = lane((128, 128)) // 32
        from_row = lax.broadcasted_iota(jnp.int32, (128, 128), 0)
        hot_y = (from_row == block * ROWS + k).astype(jnp.bfloat16)
        hot_x = (from_row == block + k * BLOCKS).astype(jnp.bfloat16)
        wide_y = jnp.dot(turn[L : 2 * L, :].astype(jnp.bfloat16), hot_y, preferred_element_type=jnp.float32)
        wide_x = jnp.dot(turn[3 * L : 4 * L, :].astype(jnp.bfloat16), hot_x, preferred_element_type=jnp.float32)
        scale_x[k] = jnp.where(wide_y > 0.5, DOWN, UP)
        scale_y[k] = jnp.where(wide_x > 0.5, DOWN, UP)
        return carry

    lax.fori_loop(0, ROWS, spread, 0)

    def wait_blocks(sem, buffer, count):
        blocks = buffer.at[pl.ds(0, count)]
        pltpu.make_async_remote_copy(
            src_ref=blocks,
            dst_ref=blocks,
            send_sem=send_sem,
            recv_sem=sem,
            device_id={"cols": lax.rem(me + 1, PEERS)},
            device_id_type=MESH,
        ).wait_recv()

    def wait_group(sem, buffer, step, count, own):
        @pl.when(step == 0)
        def _():
            wait_blocks(sem, buffer, count - own)

        @pl.when(step != 0)
        def _():
            wait_blocks(sem, buffer, count)

    group = GROUP

    def right_half(half, carry):
        weights = right_ref[...]

        def store_lines(spots, tiles):
            for spot, rows in zip(spots, tiles):
                for k, tile in enumerate(tiles_of_rows(rows)):
                    lines[pl.ds(spot * BLOCKS + k, ROWS, stride=PITCH_X), :] = tile

        def by_lines(step, carry):
            spots = [lax.rem(me // BLOCKS + 2 * ROWS - step * group - k, ROWS) for k in range(group)]
            wait_group(recv_sems.at[half * 2 + step], arrived, step, group * BLOCKS, 1)
            tiles = [
                rows_of_tiles([arrived[half * PEERS + spot * BLOCKS + k] for k in range(BLOCKS)]) for spot in spots
            ]
            store_lines(spots, mix_tiles(weights, tiles))
            return carry

        lax.fori_loop(0, ROWS // group, by_lines, 0)

        def across(step, carry):
            spots = [step * group + k for k in range(group)]
            tiles = [lines[pl.ds(pl.multiple_of(spot * PITCH_X, 8), L), :] for spot in spots]
            tiles = mix_tiles(weights, tiles)
            tiles = mix_tiles(weights, [tile * scale_x[spot] for spot, tile in zip(spots, tiles)])
            for spot, tile in zip(spots, tiles):
                lines[pl.ds(pl.multiple_of(spot * PITCH_X, 8), L), :] = tile
            return carry

        lax.fori_loop(0, ROWS // group, across, 0)

        def along(step, carry):
            spots = [step * group + k for k in range(group)]
            tiles = [
                rows_of_tiles([lines[pl.ds(spot * BLOCKS + k, ROWS, stride=PITCH_X), :] for k in range(BLOCKS)])
                for spot in spots
            ]
            tiles = mix_tiles(weights, tiles)
            tiles = mix_tiles(weights, [tile * scale_y[spot] for spot, tile in zip(spots, tiles)])
            store_lines(spots, tiles)
            return carry

        lax.fori_loop(0, ROWS // group, along, 0)

        def finish(step, carry):
            spots = [step * group + k for k in range(group)]
            tiles = [lines[pl.ds(pl.multiple_of(spot * PITCH_X, 8), L), :] for spot in spots]
            for spot, tile in zip(spots, mix_tiles(weights, tiles)):
                returning[pl.ds(half * PEERS * PITCH_OUT + spot, L, stride=PITCH_OUT), :] = tile
            return carry

        lax.fori_loop(0, ROWS // group, finish, 0)

        def send_back(k, carry):
            peer = lax.rem(me + k, PEERS)
            pltpu.make_async_remote_copy(
                src_ref=returning.at[pl.ds(pl.multiple_of((half * PEERS + peer) * PITCH_OUT, 8), ROWS), :],
                dst_ref=landed.at[half * PEERS + me],
                send_sem=back_send_sem,
                recv_sem=back_recv_sems.at[lax.rem(peer // 2 + TILES - me // 2, TILES) // MERGED],
                device_id={"cols": peer},
                device_id_type=MESH,
            ).start()
            return carry

        lax.fori_loop(1, PEERS, send_back, 0)
        landed[half * PEERS + me] = returning[pl.ds(pl.multiple_of((half * PEERS + me) * PITCH_OUT, 8), ROWS), :]
        return carry

    lax.fori_loop(0, HALVES, right_half, 0)

    def merge(step, carry):
        spots = [lax.rem(me // 2 + 2 * TILES - step * MERGED - k, TILES) for k in range(MERGED)]
        wait_group(back_recv_sems.at[step], landed, step, MERGED * 2 * HALVES, HALVES)
        for spot in spots:
            tiles = [landed[half * PEERS + 2 * spot + q] for q in range(2) for half in range(HALVES)]
            columns = pl.ds(pl.multiple_of(spot * 128, 128), 128)
            for k, tile in enumerate(swap_blocks(tiles)):
                out_ref[k * ROWS : (k + 1) * ROWS, columns] = tile
        return carry

    lax.fori_loop(0, TILES // MERGED, merge, 0)

    for buffer, sem in ((arrived, send_sem), (landed, back_send_sem)):
        everything = buffer.at[pl.ds(0, HALVES * (PEERS - 1))]
        pltpu.make_async_remote_copy(
            src_ref=everything,
            dst_ref=everything,
            send_sem=sem,
            recv_sem=recv_sems.at[0],
            device_id={"cols": lax.rem(me + 1, PEERS)},
            device_id_type=MESH,
        ).wait_send()


def shards(green_by_column, field):
    green = green_by_column.reshape(L, SITES)
    bits = field.reshape(SLICES * TILES, 128)
    order = np.concatenate([np.arange(0, L, 2), np.arange(1, L, 2)])
    columns = np.arange(128).reshape(2, HALVES, 32).transpose(1, 0, 2).reshape(128)
    forward = circulant(hop_rate)
    inverse = circulant(-hop_rate)
    narrow = np.concatenate(
        [as_left(forward[np.ix_(order, order)]), as_left(forward[:, order]), as_left(inverse)], axis=0
    )
    wide = np.concatenate([as_right(forward, np.arange(128)), as_right(forward, columns)], axis=0)
    vmem = pl.BlockSpec(memory_space=pltpu.VMEM)
    wrapped = pl.pallas_call(
        kernel,
        out_shape=pltpu.VMEM((L, SITES), jnp.float32),
        in_specs=[pl.BlockSpec(memory_space=pl.ANY)] * 4,
        out_specs=vmem,
        scratch_shapes=[
            pltpu.VMEM((SLICES * TILES, 128), jnp.int32),
            pltpu.VMEM(narrow.shape, jnp.bfloat16),
            pltpu.VMEM(wide.shape, jnp.bfloat16),
            pltpu.VMEM((TILES * PITCH_IN, 128), jnp.float32),
            pltpu.VMEM((SLICES * L, 128), jnp.float32),
            pltpu.VMEM((4 * L, 128), jnp.float32),
            pltpu.VMEM((ROWS, 128), jnp.float32),
            pltpu.VMEM((ROWS, L, 128), jnp.float32),
            pltpu.VMEM((ROWS, L, 128), jnp.float32),
            pltpu.VMEM((HALVES * PEERS * PITCH_OUT, 128), jnp.float32),
            pltpu.VMEM((HALVES * PEERS, ROWS, 128), jnp.float32),
            pltpu.VMEM((ROWS * PITCH_X, 128), jnp.float32),
            pltpu.VMEM((HALVES * PEERS * PITCH_OUT, 128), jnp.float32),
            pltpu.VMEM((HALVES * PEERS, ROWS, 128), jnp.float32),
            pltpu.SemaphoreType.DMA((3,)),
            pltpu.SemaphoreType.DMA,
            pltpu.SemaphoreType.DMA,
            pltpu.SemaphoreType.DMA((HALVES * ROWS // GROUP,)),
            pltpu.SemaphoreType.DMA,
            pltpu.SemaphoreType.DMA((TILES // MERGED,)),
        ],
        compiler_params=pltpu.CompilerParams(collective_id=0, has_side_effects=True),
    )(green, bits, jnp.asarray(narrow), jnp.asarray(wide))
    return wrapped.reshape(1, L, SITES)


def solution(mesh):
    return jax.shard_map(
        shards,
        mesh=mesh,
        in_specs=(P("walk", "cols", None), P("walk", None, None)),
        out_specs=P("walk", "cols", None),
        check_vma=False,
    )
```

```python
import jax
import jax.numpy as jnp
import numpy as np
from jax import lax
from jax.experimental import pallas as pl
from jax.experimental.pallas import tpu as pltpu
from jax.sharding import PartitionSpec as P

L = 64
SITES = L * L
SLICES = 3
PEERS = 64
TILES = SITES // 128
BLOCKS = 4
ROWS = L // BLOCKS
HALVES = 2
STEPS = 2
PER_STEP = ROWS // STEPS
GROUP = 8
MERGED = 4
PITCH_IN = 72
PITCH_OUT = 24
PITCH_X = 72

hop_rate = 0.6
coupling = 0.65373
UP = float(np.exp(coupling))
DOWN = float(np.exp(-coupling))

MESH = pl.DeviceIdType.MESH


def circulant(rate):
    k = np.arange(L)
    spectrum = np.exp(rate * np.cos(2.0 * np.pi * k / L))
    differ = k[:, None] - k[None, :]
    waves = np.cos(2.0 * np.pi * (differ[:, :, None] * k) / L)
    return (waves * spectrum).sum(-1) / L


def high_low(matrix):
    matrix = matrix.astype(np.float32)
    high = matrix.astype(jnp.bfloat16)
    low = (matrix - high.astype(np.float32)).astype(jnp.bfloat16)
    return high, low


def as_left(matrix):
    high, low = high_low(matrix)
    return np.concatenate([high, low, high], axis=1)


def as_right(matrix, columns):
    both = np.kron(np.eye(2), matrix)[:, columns]
    high, low = high_low(both)
    upper = np.concatenate([high, low], axis=1)
    lower = np.concatenate([high, np.zeros_like(low)], axis=1)
    return np.concatenate([upper, lower], axis=0)


def split(values):
    high = values.astype(jnp.bfloat16)
    low = (values - high.astype(jnp.float32)).astype(jnp.bfloat16)
    return high, low


def mix_rows(weights, values):
    high, low = split(values)
    stacked = jnp.concatenate([high, high, low], axis=0)
    return jnp.dot(weights, stacked, preferred_element_type=jnp.float32)


def mix_lanes(values, weights):
    high, low = split(values)
    wide = jnp.concatenate([high, low], axis=1)
    both = jnp.dot(wide, weights, preferred_element_type=jnp.float32)
    return both[:, :128] + both[:, 128:]


def lane(shape):
    return lax.broadcasted_iota(jnp.int32, shape, len(shape) - 1)


def swap_lanes(first, second, width):
    keep = (lane(first.shape) // width) % 2 == 0
    return (
        jnp.where(keep, first, pltpu.roll(second, width, 1)),
        jnp.where(keep, pltpu.roll(first, 128 - width, 1), second),
    )


def swap_blocks(tiles):
    t0, t2 = swap_lanes(tiles[0], tiles[2], 64)
    t1, t3 = swap_lanes(tiles[1], tiles[3], 64)
    t0, t1 = swap_lanes(t0, t1, 32)
    t2, t3 = swap_lanes(t2, t3, 32)
    return [t0, t1, t2, t3]


def rows_of_tiles(tiles):
    return jnp.concatenate(swap_blocks(tiles), axis=0)


def tiles_of_rows(rows):
    return swap_blocks([rows[k * ROWS : (k + 1) * ROWS] for k in range(BLOCKS)])


def beside(tiles):
    return jnp.concatenate(tiles, axis=1)


def mix_tiles(weights, tiles):
    mixed = [mix_rows(weights, beside(tiles[k : k + 2])) for k in range(0, len(tiles), 2)]
    return [half for pair in mixed for half in (pair[:, :128], pair[:, 128:])]


def kernel(
    green_ref, field_hbm, left_hbm, last_hbm, lanes_hbm, lanes_last_hbm, right_hbm, out_ref,
    field_ref, left_ref, last_ref, lanes_ref, lanes_last_ref, right_ref, held, gain, turn, own_scale, scale_x, scale_y,
    outgoing, arrived, lines, returning, landed,
    small_sems, load_sem, send_sem, recv_sems, back_send_sem, back_recv_sems,
):
    me = lax.axis_index("cols")
    barrier = pltpu.get_barrier_semaphore()

    def greet(k, carry):
        pl.semaphore_signal(
            barrier, inc=1, device_id={"cols": lax.rem(me + k, PEERS)}, device_id_type=MESH
        )
        return carry

    for k in range(1, PEERS):
        greet(k, 0)

    loads = [
        pltpu.make_async_copy(
            green_ref.at[:, pl.ds(t * 128, 128)],
            held.at[pl.ds(t * PITCH_IN, L), :],
            load_sem,
        )
        for t in range(TILES)
    ]
    smalls = [
        pltpu.make_async_copy(source, target, small_sems.at[k])
        for k, (source, target) in enumerate(
            [
                (field_hbm, field_ref),
                (left_hbm, left_ref),
                (lanes_hbm, lanes_ref),
                (last_hbm, last_ref),
                (lanes_last_hbm, lanes_last_ref),
                (right_hbm, right_ref),
            ]
        )
    ]
    smalls[0].start()
    for load in loads:
        load.start()
    for small in smalls[1:]:
        small.start()

    smalls[0].wait()
    low_half = lane((TILES, 128)) < 64
    for moment in range(SLICES):
        bits = field_ref[moment * TILES : (moment + 1) * TILES, :].astype(jnp.float32)
        turned = pltpu.roll(bits, 64, 1)
        even = jnp.where(low_half, bits, turned)
        odd = jnp.where(low_half, turned, bits)
        gain[moment * L : moment * L + TILES, :] = jnp.where(even > 0.5, UP, DOWN)
        gain[moment * L + TILES : (moment + 1) * L, :] = jnp.where(odd > 0.5, UP, DOWN)
        turn[pl.ds(moment * L, TILES, stride=2), :] = bits
        turn[pl.ds(moment * L + 1, TILES, stride=2), :] = turned
    mine = jnp.broadcast_to(turn[pl.ds(me, 1), :], (ROWS, 128))
    site = lane((ROWS, 128))
    spot_row = lax.broadcasted_iota(jnp.int32, (ROWS, 128), 0)
    own_bits = jnp.zeros((ROWS, 128), jnp.float32)
    for block in range(BLOCKS):
        picked = jnp.where(site == spot_row + block * ROWS, mine, 0.0)
        own_bits = jnp.where(site // 32 == block, jnp.sum(picked, axis=1, keepdims=True), own_bits)
    own_scale[...] = jnp.where(own_bits > 0.5, DOWN, UP)

    for small in smalls[1:]:
        small.wait()
    pltpu.make_async_copy(arrived, arrived, load_sem).wait()

    def send_out(half, start, count):
        def one(k, carry):
            peer = lax.rem(me + k, PEERS)
            pltpu.make_async_remote_copy(
                src_ref=outgoing.at[pl.ds(pl.multiple_of((half * PEERS + peer) * PITCH_OUT + start, 8), count), :],
                dst_ref=arrived.at[half * PEERS + me, pl.ds(pl.multiple_of(start, 8), count), :],
                send_sem=send_sem,
                recv_sem=recv_sems.at[half * 2 + lax.rem(peer // BLOCKS + ROWS - me // BLOCKS, ROWS) // GROUP],
                device_id={"cols": peer},
                device_id_type=MESH,
            ).start()
            return carry

        lax.fori_loop(1, PEERS, one, 0)

    def left_step(step, carry):
        base = step * PER_STEP
        tiles = []
        for k in range(PER_STEP):
            for upper in range(2):
                row = base + k + upper * 2 * ROWS
                pair = swap_lanes(
                    held[pl.ds(row, TILES, stride=PITCH_IN), :],
                    held[pl.ds(row + ROWS, TILES, stride=PITCH_IN), :],
                    64,
                )
                tiles.append(jnp.concatenate(pair, axis=0))
        for moment in range(SLICES):
            ends = moment == SLICES - 1
            scale = gain[moment * L : (moment + 1) * L, :]
            tiles = mix_tiles((last_ref if ends else left_ref)[...], [tile * scale for tile in tiles])
            weights = (lanes_last_ref if ends else lanes_ref)[...]
            stack = mix_lanes(jnp.concatenate(tiles, axis=0), weights)
            tiles = [stack[k * L : (k + 1) * L] for k in range(len(tiles))]
        for k in range(PER_STEP):
            row = own_scale[pl.ds(base + k, 1), :]
            for half, tile in enumerate(swap_lanes(tiles[2 * k], tiles[2 * k + 1], 64)):
                outgoing[pl.ds(half * PEERS * PITCH_OUT + base + k, L, stride=PITCH_OUT), :] = tile * row

        @pl.when(step == 0)
        def _():
            pl.semaphore_wait(barrier, PEERS - 1)

        send_out(0, base, PER_STEP)
        return carry

    lax.fori_loop(0, STEPS, left_step, 0)
    send_out(1, 0, ROWS)

    for half in range(HALVES):
        arrived[half * PEERS + me] = outgoing[pl.ds(pl.multiple_of((half * PEERS + me) * PITCH_OUT, 8), ROWS), :]

    square = jnp.concatenate([turn[2 * L : 3 * L, :], jnp.zeros((L, 128), jnp.float32)], axis=0)
    turn[3 * L : 4 * L, :] = square.T[:L, :]

    def spread(k, carry):
        block = lane((128, 128)) // 32
        from_row = lax.broadcasted_iota(jnp.int32, (128, 128), 0)
        hot_y = (from_row == block * ROWS + k).astype(jnp.bfloat16)
        hot_x = (from_row == block + k * BLOCKS).astype(jnp.bfloat16)
        wide_y = jnp.dot(turn[L : 2 * L, :].astype(jnp.bfloat16), hot_y, preferred_element_type=jnp.float32)
        wide_x = jnp.dot(turn[3 * L : 4 * L, :].astype(jnp.bfloat16), hot_x, preferred_element_type=jnp.float32)
        scale_x[k] = jnp.where(wide_y > 0.5, DOWN, UP)
        scale_y[k] = jnp.where(wide_x > 0.5, DOWN, UP)
        return carry

    lax.fori_loop(0, ROWS, spread, 0)

    def wait_blocks(sem, buffer, count):
        blocks = buffer.at[pl.ds(0, count)]
        pltpu.make_async_remote_copy(
            src_ref=blocks,
            dst_ref=blocks,
            send_sem=send_sem,
            recv_sem=sem,
            device_id={"cols": lax.rem(me + 1, PEERS)},
            device_id_type=MESH,
        ).wait_recv()

    def wait_group(sem, buffer, step, count, own):
        @pl.when(step == 0)
        def _():
            wait_blocks(sem, buffer, count - own)

        @pl.when(step != 0)
        def _():
            wait_blocks(sem, buffer, count)

    group = GROUP

    def right_half(half, carry):
        weights = right_ref[...]

        def store_lines(spots, tiles):
            for spot, rows in zip(spots, tiles):
                for k, tile in enumerate(tiles_of_rows(rows)):
                    lines[pl.ds(spot * BLOCKS + k, ROWS, stride=PITCH_X), :] = tile

        def by_lines(step, carry):
            spots = [lax.rem(me // BLOCKS + 2 * ROWS - step * group - k, ROWS) for k in range(group)]
            wait_group(recv_sems.at[half * 2 + step], arrived, step, group * BLOCKS, 1)
            tiles = [
                rows_of_tiles([arrived[half * PEERS + spot * BLOCKS + k] for k in range(BLOCKS)]) for spot in spots
            ]
            store_lines(spots, mix_tiles(weights, tiles))
            return carry

        lax.fori_loop(0, ROWS // group, by_lines, 0)

        def across(step, carry):
            spots = [step * group + k for k in range(group)]
            tiles = [lines[pl.ds(pl.multiple_of(spot * PITCH_X, 8), L), :] for spot in spots]
            tiles = mix_tiles(weights, tiles)
            tiles = mix_tiles(weights, [tile * scale_x[spot] for spot, tile in zip(spots, tiles)])
            for spot, tile in zip(spots, tiles):
                lines[pl.ds(pl.multiple_of(spot * PITCH_X, 8), L), :] = tile
            return carry

        lax.fori_loop(0, ROWS // group, across, 0)

        def along(step, carry):
            spots = [step * group + k for k in range(group)]
            tiles = [
                rows_of_tiles([lines[pl.ds(spot * BLOCKS + k, ROWS, stride=PITCH_X), :] for k in range(BLOCKS)])
                for spot in spots
            ]
            tiles = mix_tiles(weights, tiles)
            tiles = mix_tiles(weights, [tile * scale_y[spot] for spot, tile in zip(spots, tiles)])
            store_lines(spots, tiles)
            return carry

        lax.fori_loop(0, ROWS // group, along, 0)

        def finish(step, carry):
            spots = [step * group + k for k in range(group)]
            tiles = [lines[pl.ds(pl.multiple_of(spot * PITCH_X, 8), L), :] for spot in spots]
            for spot, tile in zip(spots, mix_tiles(weights, tiles)):
                returning[pl.ds(half * PEERS * PITCH_OUT + spot, L, stride=PITCH_OUT), :] = tile
            return carry

        lax.fori_loop(0, ROWS // group, finish, 0)

        def send_back(k, carry):
            peer = lax.rem(me + k, PEERS)
            pltpu.make_async_remote_copy(
                src_ref=returning.at[pl.ds(pl.multiple_of((half * PEERS + peer) * PITCH_OUT, 8), ROWS), :],
                dst_ref=landed.at[half * PEERS + me],
                send_sem=back_send_sem,
                recv_sem=back_recv_sems.at[lax.rem(peer // 2 + TILES - me // 2, TILES) // MERGED],
                device_id={"cols": peer},
                device_id_type=MESH,
            ).start()
            return carry

        lax.fori_loop(1, PEERS, send_back, 0)
        landed[half * PEERS + me] = returning[pl.ds(pl.multiple_of((half * PEERS + me) * PITCH_OUT, 8), ROWS), :]
        return carry

    lax.fori_loop(0, HALVES, right_half, 0)

    def merge(step, carry):
        spots = [lax.rem(me // 2 + 2 * TILES - step * MERGED - k, TILES) for k in range(MERGED)]
        wait_group(back_recv_sems.at[step], landed, step, MERGED * 2 * HALVES, HALVES)
        for spot in spots:
            tiles = [landed[half * PEERS + 2 * spot + q] for q in range(2) for half in range(HALVES)]
            columns = pl.ds(pl.multiple_of(spot * 128, 128), 128)
            for k, tile in enumerate(swap_blocks(tiles)):
                out_ref[k * ROWS : (k + 1) * ROWS, columns] = tile
        return carry

    lax.fori_loop(0, TILES // MERGED, merge, 0)

    for buffer, sem in ((arrived, send_sem), (landed, back_send_sem)):
        everything = buffer.at[pl.ds(0, HALVES * (PEERS - 1))]
        pltpu.make_async_remote_copy(
            src_ref=everything,
            dst_ref=everything,
            send_sem=sem,
            recv_sem=recv_sems.at[0],
            device_id={"cols": lax.rem(me + 1, PEERS)},
            device_id_type=MESH,
        ).wait_send()


def shards(green_by_column, field):
    green = green_by_column.reshape(L, SITES)
    bits = field.reshape(SLICES * TILES, 128)
    order = np.concatenate([np.arange(0, L, 2), np.arange(1, L, 2)])
    columns = np.arange(128).reshape(2, HALVES, 32).transpose(1, 0, 2).reshape(128)
    forward = circulant(hop_rate)
    inverse = circulant(-hop_rate)
    left = jnp.asarray(as_left(forward[np.ix_(order, order)]))
    last = jnp.asarray(as_left(forward[:, order]))
    lanes = jnp.asarray(as_right(forward, np.arange(128)))
    lanes_last = jnp.asarray(as_right(forward, columns))
    right = jnp.asarray(as_left(inverse))
    vmem = pl.BlockSpec(memory_space=pltpu.VMEM)
    wrapped = pl.pallas_call(
        kernel,
        out_shape=pltpu.VMEM((L, SITES), jnp.float32),
        in_specs=[pl.BlockSpec(memory_space=pl.ANY)] * 7,
        out_specs=vmem,
        scratch_shapes=[
            pltpu.VMEM((SLICES * TILES, 128), jnp.int32),
            pltpu.VMEM(left.shape, jnp.bfloat16),
            pltpu.VMEM(last.shape, jnp.bfloat16),
            pltpu.VMEM(lanes.shape, jnp.bfloat16),
            pltpu.VMEM(lanes_last.shape, jnp.bfloat16),
            pltpu.VMEM(right.shape, jnp.bfloat16),
            pltpu.VMEM((TILES * PITCH_IN, 128), jnp.float32),
            pltpu.VMEM((SLICES * L, 128), jnp.float32),
            pltpu.VMEM((4 * L, 128), jnp.float32),
            pltpu.VMEM((ROWS, 128), jnp.float32),
            pltpu.VMEM((ROWS, L, 128), jnp.float32),
            pltpu.VMEM((ROWS, L, 128), jnp.float32),
            pltpu.VMEM((HALVES * PEERS * PITCH_OUT, 128), jnp.float32),
            pltpu.VMEM((HALVES * PEERS, ROWS, 128), jnp.float32),
            pltpu.VMEM((ROWS * PITCH_X, 128), jnp.float32),
            pltpu.VMEM((HALVES * PEERS * PITCH_OUT, 128), jnp.float32),
            pltpu.VMEM((HALVES * PEERS, ROWS, 128), jnp.float32),
            pltpu.SemaphoreType.DMA((6,)),
            pltpu.SemaphoreType.DMA,
            pltpu.SemaphoreType.DMA,
            pltpu.SemaphoreType.DMA((HALVES * ROWS // GROUP,)),
            pltpu.SemaphoreType.DMA,
            pltpu.SemaphoreType.DMA((TILES // MERGED,)),
        ],
        compiler_params=pltpu.CompilerParams(collective_id=0, has_side_effects=True),
    )(green, bits, left, last, lanes, lanes_last, right)
    return wrapped.reshape(1, L, SITES)


def solution(mesh):
    return jax.shard_map(
        shards,
        mesh=mesh,
        in_specs=(P("walk", "cols", None), P("walk", None, None)),
        out_specs=P("walk", "cols", None),
        check_vma=False,
    )
```
